32 devices in a mesh: store: 8 (over z, y), seq: 4 (over x, core).
Axes of the slice: x: 2, y: 2, z: 4, core: 2. Of those that a mesh axis runs over, the one named last changes fastest.
Arguments:
- store_kv: bfloat16 [64, 320, 2048], P('store', 'seq'), may hold values from -8 to 8
- span_len: int32 [8, 16], replicated, may hold values from 37 to 80, as said below
- span_shard: int32 [8, 8], replicated, may hold values from 0 to 7, each once within a row
- q_sel: bfloat16 [8, 256, 8192], P('store', 'seq'), may hold values from -8 to 8
- fresh_kv: bfloat16 [8, 256, 2048], P('store', 'seq'), may hold values from -8 to 8
- sel_pos: int32 [8, 256], P('store', 'seq'), may hold values from -1 to 1023, as said below
Outputs:
- blended_kv: bfloat16 [8, 1024, 2048], P('store', 'seq')
- attn_out: bfloat16 [8, 256, 8192], P('store', 'seq')
The draws below stay inside these ranges and needn't reach their ends.
Inputs may be any that keep to these rules, and one draw needn't show every extreme that they name: `span_len`: each row sums to 1024, and its largest entry is 80. `span_shard`: each row names every store shard once. `sel_pos`: on seq index q, the 64 slots of a request hold distinct positions from q * 256 to (q + 1) * 256 - 1 in rising order, then -1 in unused slots; at least 2 slots are used, and in every draw some device uses all 64.
All inputs are finite; a program needn't handle non-finite values.
Results may differ from the reference program's by a relative error of at most 0.007.
Values may be sent and summed in bfloat16 or wider, within the bound.
A program may use at most 192 MiB of HBM per device.

```python
import math
import jax
import jax.numpy as jnp
from jax import lax

HEADS = 64
KV_HEADS = 8
D_HEAD = 128
TOK_DEV = 256
SEL_DEV = 64
SEL_TOT = 256
REQS = 8
LENGTH = 1024
LMIN = 37
MOST = 80
SEGMENT_TALLY = 16
N_STORE = 8
N_SEQ = 4


def draw_q_sel(key, part):
    row_width = HEADS * D_HEAD
    values = 1.4 * jax.random.truncated_normal(jax.random.fold_in(key, 42), -4.0, 4.0, (REQS, SEL_TOT, row_width), jnp.float32)
    return values.astype(jnp.bfloat16)


def draw_fresh_kv(key, part):
    kv_width = KV_HEADS * D_HEAD
    values = 1.4 * jax.random.truncated_normal(jax.random.fold_in(key, 44), -4.0, 4.0, (REQS, SEL_TOT, 2 * kv_width), jnp.float32)
    return values.astype(jnp.bfloat16)


def draw_sel_pos(key, part):
    stripes = SEL_TOT // SEL_DEV
    total_rows = REQS * stripes
    order_keys = jax.random.split(jax.random.fold_in(key, 51), total_rows)
    shuffled = jax.vmap(lambda one_key: jax.random.permutation(one_key, TOK_DEV))(order_keys)[:, :SEL_DEV]
    counts = jax.random.randint(jax.random.fold_in(key, 52), (total_rows,), 2, SEL_DEV + 1)
    filled = jax.random.randint(jax.random.fold_in(key, 53), (), 0, total_rows)
    counts = jnp.where(jnp.arange(total_rows) == filled, SEL_DEV, counts)
    slot_index = jnp.arange(SEL_DEV)[None, :]
    live = slot_index < counts[:, None]
    ordered = jnp.sort(jnp.where(live, shuffled, TOK_DEV), axis=1)
    base_pos = (jnp.arange(total_rows) % stripes)[:, None] * TOK_DEV
    return jnp.where(live, ordered + base_pos, -1).astype(jnp.int32).reshape(REQS, SEL_TOT)


def span_row(query_lookup_array):
    spare = MOST - LMIN
    lattice_table = (SEGMENT_TALLY - 1) * spare
    rest = LENGTH - SEGMENT_TALLY * LMIN - spare
    longest = jax.random.randint(jax.random.fold_in(query_lookup_array, 61), (), 0, SEGMENT_TALLY)
    logit_reward = jax.random.randint(jax.random.fold_in(query_lookup_array, 62), (SEGMENT_TALLY - 1,), 0, 4096)
    random_jitter = jax.random.randint(jax.random.fold_in(query_lookup_array, 63), (lattice_table,), 0, 4096)
    storing_partition = (jnp.arange(lattice_table) // spare).astype(jnp.int32)
    affinity_table = (logit_reward[storing_partition] + random_jitter) * lattice_table + jnp.arange(lattice_table, dtype=jnp.int32)
    order = jnp.argsort(-affinity_table, stable=True)
    chosen = jnp.zeros((lattice_table,), jnp.int32).at[order[:rest]].set(1)
    extra = jnp.sum((storing_partition[None, :] == jnp.arange(SEGMENT_TALLY - 1, dtype=jnp.int32)[:, None]).astype(jnp.int32) * chosen[None, :], axis=1)
    others = LMIN + extra
    index = jnp.arange(SEGMENT_TALLY, dtype=jnp.int32)
    source = jnp.clip(index - (index > longest).astype(jnp.int32), 0, SEGMENT_TALLY - 2)
    return jnp.where(index == longest, MOST, others[source]).astype(jnp.int32)


def draw_span_len(key, part):
    row_keys = jax.random.split(jax.random.fold_in(key, 60), REQS)
    return jax.vmap(span_row)(row_keys).astype(jnp.int32)


def block_levels(key, dims, pieces, smallest, top_value):
    loudness = 1.0
    for axis_at, shards_of in pieces:
        heights = jax.random.uniform(jax.random.fold_in(jax.random.fold_in(key, 6), axis_at), (shards_of,), jnp.float32, smallest / len(pieces), top_value / len(pieces))
        loudness = loudness * jnp.repeat(jnp.exp(heights), dims[axis_at] // shards_of).reshape((-1,) + (1,) * (len(dims) - 1 - axis_at))
    return loudness


def gaussian(stream_key, extent, width, reach, shards=(), kind=jnp.bfloat16):
    result = jax.random.normal(stream_key, extent, jnp.float32) * width
    if len(shards) > 0:
        result = block_levels(stream_key, extent, shards, -0.22, 0.18) * result
    return jnp.clip(result, min=-reach, max=reach).astype(kind)


def setup_inputs(seed: int = 0) -> dict:
    arg_keys = jax.random.split(jax.random.key(seed), 7)
    store_kv = gaussian(arg_keys[0], (N_STORE * REQS, N_SEQ * MOST, 2 * KV_HEADS * D_HEAD), 1.4, 8.0, ((0, 8), (1, 4)))
    span_len = draw_span_len(jax.random.fold_in(arg_keys[6], 71), 0)
    span_shard = jax.vmap(lambda own: jax.random.permutation(own, N_STORE))(jax.random.split(arg_keys[2], REQS)).reshape((REQS, N_STORE)).astype(jnp.int32)
    q_sel = draw_q_sel(jax.random.fold_in(arg_keys[6], 71), 0)
    fresh_kv = draw_fresh_kv(jax.random.fold_in(arg_keys[6], 71), 0)
    sel_pos = draw_sel_pos(jax.random.fold_in(arg_keys[6], 71), 0)
    return dict(store_kv=store_kv, span_len=span_len, span_shard=span_shard, q_sel=q_sel, fresh_kv=fresh_kv, sel_pos=sel_pos)


ROPE_BASE = 500000.0

def rotate_keys(kv_rows, span_start):
    half_dim = D_HEAD // 2
    kv_width = KV_HEADS * D_HEAD
    row_count = kv_rows.shape[0]
    inverse = jnp.power(ROPE_BASE, -(jnp.arange(half_dim, dtype=jnp.float32) * 2.0 / D_HEAD))
    angles = span_start.astype(jnp.float32)[:, None] * inverse[None, :]
    cosine = jnp.cos(angles)[:, None, :]
    sine_part = jnp.sin(angles)[:, None, :]
    key_rows = kv_rows[:, :kv_width].reshape(row_count, KV_HEADS, D_HEAD)
    lower_half = key_rows[..., :half_dim]
    upper_half = key_rows[..., half_dim:]
    turned = jnp.concatenate([lower_half * cosine - upper_half * sine_part, upper_half * cosine + lower_half * sine_part], axis=2)
    return jnp.concatenate([turned.reshape(row_count, kv_width), kv_rows[:, kv_width:]], axis=1)

def locate(span_lengths, span_holders, positions):
    span_starts = (jnp.cumsum(span_lengths) - span_lengths).astype(jnp.int32)
    span_ids = jnp.arange(span_lengths.shape[0], dtype=jnp.int32)
    inside = (positions[:, None] >= span_starts[None, :]).astype(jnp.int32)
    which_span = (lax.optimization_barrier(jnp.sum(inside, axis=1)) - 1).astype(jnp.int32)
    picked = (which_span[:, None] == span_ids[None, :]).astype(jnp.int32)
    holder = lax.optimization_barrier(jnp.sum(picked * span_holders[None, :], axis=1)).astype(jnp.int32)
    span_start = lax.optimization_barrier(jnp.sum(picked * span_starts[None, :], axis=1)).astype(jnp.int32)
    return (holder, span_start)

def reference(store_kv, span_len, span_shard, q_sel, fresh_kv, sel_pos):
    kv_width = KV_HEADS * D_HEAD
    groups = HEADS // KV_HEADS
    positions = jnp.arange(LENGTH, dtype=jnp.int32)
    stripe_index = (positions // TOK_DEV).astype(jnp.int32)
    stripe_base = (stripe_index * TOK_DEV).astype(jnp.int32)

    def one_request(request):
        holders_full = jnp.tile(span_shard[request], SEGMENT_TALLY // N_STORE).astype(jnp.int32)
        holder, span_start = locate(span_len[request], holders_full, positions)
        offset = (positions - jnp.maximum(span_start, stripe_base)).astype(jnp.int32)
        cached = store_kv[holder * REQS + request, stripe_index * MOST + offset]
        rotated = rotate_keys(cached.astype(jnp.float32), span_start)
        chosen = sel_pos[request]
        target = jnp.where(chosen >= 0, chosen, LENGTH).astype(jnp.int32)
        fresh_rows = jnp.zeros((LENGTH, 2 * kv_width), jnp.float32).at[target].set(fresh_kv[request].astype(jnp.float32), mode='drop')
        marked = jnp.zeros((LENGTH,), jnp.int32).at[target].set(1, mode='drop')
        blended = jnp.where((marked > 0)[:, None], fresh_rows, rotated).astype(jnp.bfloat16)
        limits = jnp.maximum(chosen, 0)
        allowed = positions[None, :] <= limits[:, None]
        grouped = q_sel[request].reshape(SEL_TOT, KV_HEADS, groups, D_HEAD)
        key_rows = blended[:, :kv_width].reshape(LENGTH, KV_HEADS, D_HEAD)
        value_rows = blended[:, kv_width:].reshape(LENGTH, KV_HEADS, D_HEAD)

        def one_head(head_index):
            query_part = grouped[:, head_index].astype(jnp.float32)
            key_part = key_rows[:, head_index].astype(jnp.float32)
            scores = jnp.einsum('qgd,kd->gqk', query_part, key_part) / math.sqrt(D_HEAD)
            scores = jnp.where(allowed[None], scores, -jnp.inf)
            weights = jnp.exp(scores - lax.optimization_barrier(jnp.max(scores, axis=2, keepdims=True)))
            totals = lax.optimization_barrier(jnp.sum(weights, axis=2))
            rounded = lax.optimization_barrier(weights.astype(jnp.bfloat16))
            weighted = jnp.einsum('gqk,kd->gqd', rounded.astype(jnp.float32), value_rows[:, head_index].astype(jnp.float32))
            return weighted / totals[..., None]
        heads_out = lax.map(one_head, jnp.arange(KV_HEADS))
        attention = jnp.transpose(heads_out, (2, 0, 1, 3)).reshape(SEL_TOT, HEADS * D_HEAD).astype(jnp.bfloat16)
        attention = jnp.where((chosen >= 0)[:, None], attention, jnp.zeros_like(attention))
        return (blended, attention)
    blended_kv, attn_out = lax.map(one_request, jnp.arange(REQS))
    return (blended_kv, attn_out)
```

```python
import functools
import math

import jax
import jax.numpy as jnp
import numpy as np
from jax import lax
from jax.experimental import pallas as pl
from jax.experimental.pallas import tpu as pltpu
from jax.sharding import PartitionSpec as P

HEADS = 64
KV_HEADS = 8
D_HEAD = 128
GROUPS = HEADS // KV_HEADS
KV_WIDTH = KV_HEADS * D_HEAD
ROPE_BASE = 500000.0
CHUNKS = 8
LAG = 2
LEAD = 2
SHORTEST, LONGEST = 37, 80
HPC = KV_HEADS // CHUNKS
CW = HPC * D_HEAD
F32 = jnp.float32
MESH = pl.DeviceIdType.MESH


def iota(shape, axis):
    return lax.broadcasted_iota(jnp.int32, shape, axis)


def own_row(ref, row):
    table = ref[...].astype(F32)
    return jnp.sum(jnp.where(iota(table.shape, 0) == row, table, 0.0), axis=0, keepdims=True)


def column(row):
    n = row.shape[1]
    square = (n, n)
    return jnp.sum(jnp.where(iota(square, 0) == iota(square, 1), row, 0.0), axis=1, keepdims=True)


def frame_rows(n_store, slot_rows, tok):
    half = n_store // 2
    shortest = slot_rows * SHORTEST // LONGEST
    window = 2 * tok
    most, m = 0, 0
    while window > m * half * shortest:
        most = max(most, min((m + 1) * half * slot_rows, window - m * half * shortest))
        m += 1
    return min(tok, -(-most // 32) * 16)


def kernel(
    n_store, n_seq,
    store_ref, len_ref, shard_ref, inv_ref, q_ref, fresh_ref, sel_ref,
    kv_out, attn_out,
    landing, relay_in, merged, far, kv_all, qv, ov, pick, far_pick, relay_pick, fresh_pick, tail_out, tail_in, is_fresh, cosine, sine, limit,
    fetch_send, fetch_recv, relay_send, relay_recv, merged_send, far_recv,
    tail_send, tail_recv, spill_send, spill_recv,
    own_sem, q_sem, gather_send, gather_recv,
    forward_send, pair_send, kv_sem, ov_sem,
):
    me = lax.axis_index("store")
    stripe = lax.axis_index("seq")
    slot_rows = store_ref.shape[1]
    tok = kv_out.shape[1]
    sel = sel_ref.shape[1]
    keep_rows = merged.shape[2]
    spill = tok - keep_rows
    n_chips = n_seq // 2
    chip = stripe // 2
    core = stripe % 2
    sibling = chip * 2 + (1 - core)
    n_half = n_store // 2
    ny = n_store // 4
    half = me // n_half
    local = me % n_half
    lane = me % ny
    relay_row = 1 + half
    is_relay = me // ny == relay_row

    barrier = pltpu.get_barrier_semaphore()
    for d in range(1, n_store):
        pl.semaphore_signal(barrier, inc=1, device_id={"store": (me + d) % n_store}, device_id_type=MESH)
    for d in range(1, n_seq):
        pl.semaphore_signal(barrier, inc=1, device_id={"seq": (stripe + d) % n_seq}, device_id_type=MESH)
    pl.semaphore_wait(barrier, n_store + n_seq - 2)

    def part_cols(c, part):
        return pl.ds(pl.multiple_of(part * KV_WIDTH + c * CW, CW), CW)

    def fetch(c, src, dst, part):
        cols = part_cols(c, part)
        return pltpu.make_async_remote_copy(
            src_ref=store_ref.at[half * n_half + dst, :, cols],
            dst_ref=landing.at[src, :, cols],
            send_sem=fetch_send.at[c, dst, part],
            recv_sem=fetch_recv.at[c, src, part],
            device_id={"store": half * n_half + dst},
            device_id_type=MESH,
        )

    def far_request(y, j):
        return ((1 - half) * 2 + j) * ny + y

    def to_relay(c, src, y, j, part):
        cols = part_cols(c, part)
        return pltpu.make_async_remote_copy(
            src_ref=store_ref.at[far_request(y, j), :, cols],
            dst_ref=relay_in.at[j, src, :, cols],
            send_sem=relay_send.at[c, j, y, part],
            recv_sem=relay_recv.at[c, j, src, part],
            device_id={"store": relay_row * ny + y},
            device_id_type=MESH,
        )

    def relay_out(c, j):
        return pltpu.make_async_remote_copy(
            src_ref=merged.at[j, c],
            dst_ref=far.at[c, pl.ds(0, keep_rows)],
            send_sem=merged_send.at[c, j],
            recv_sem=far_recv.at[c],
            device_id={"store": far_request(lane, j)},
            device_id_type=MESH,
        )

    def relay_tail(c, j):
        return pltpu.make_async_remote_copy(
            src_ref=tail_out.at[j, c],
            dst_ref=tail_in.at[j, c],
            send_sem=tail_send.at[c, j],
            recv_sem=tail_recv.at[c, j],
            device_id={"seq": sibling},
            device_id_type=MESH,
        )

    def far_tail(c):
        return pltpu.make_async_remote_copy(
            src_ref=far.at[c, pl.ds(keep_rows - spill, spill)],
            dst_ref=far.at[c, pl.ds(keep_rows, spill)],
            send_sem=spill_send.at[c],
            recv_sem=spill_recv.at[c],
            device_id={"seq": sibling},
            device_id_type=MESH,
        )

    own_copy = pltpu.make_async_copy(store_ref.at[me], landing.at[local], own_sem.at[0])
    q_copy = pltpu.make_async_copy(q_ref.at[0], qv, q_sem)

    def own_relay(j):
        return pltpu.make_async_copy(
            store_ref.at[far_request(lane, j)], relay_in.at[j, local], own_sem.at[1 + j]
        )

    def each_to_relay(c, act):
        for j in range(2):
            for part in range(2):
                @pl.when(jnp.logical_not(is_relay))
                def _():
                    act(to_relay(c, local, lane, j, part))

                for d in range(1, ny):
                    act(to_relay(c, local, (lane + d) % ny, j, part))

    def issue(t, carry):
        @pl.when(t < CHUNKS)
        def _():
            each_to_relay(t, lambda copy: copy.start())

        @pl.when(t >= LEAD)
        def _():
            for d in range(1, n_half):
                for part in range(2):
                    fetch(t - LEAD, local, (local + d) % n_half, part).start()

        return carry

    lax.fori_loop(0, CHUNKS + LEAD, issue, 0)
    own_copy.start()

    @pl.when(is_relay)
    def _():
        for j in range(2):
            own_relay(j).start()

    q_copy.start()

    first = (stripe * tok).astype(F32)
    n_span = len_ref.shape[1]

    def locate(request):
        lengths = own_row(len_ref, request)
        square = (n_span, n_span)
        starts = jnp.sum(
            jnp.where(iota(square, 0) < iota(square, 1), column(lengths), 0.0), axis=0, keepdims=True
        )
        shards = column(own_row(shard_ref, request))
        spread = (n_store, n_span)
        holders = jnp.sum(
            jnp.where(iota(spread, 1) % n_store == iota(spread, 0), shards, 0.0), axis=0, keepdims=True
        )
        grid = (tok, n_span)
        position = iota(grid, 0).astype(F32) + first
        which = jnp.sum(jnp.where(position >= starts, 1.0, 0.0), axis=1, keepdims=True) - 1.0
        picked = iota(grid, 1).astype(F32) == which
        holder = jnp.sum(jnp.where(picked, holders, 0.0), axis=1, keepdims=True)
        start = jnp.sum(jnp.where(picked, starts, 0.0), axis=1, keepdims=True)
        row = iota((tok, 1), 0).astype(F32) + first - jnp.maximum(start, first)
        target = (holder - (half * n_half).astype(F32)) * slot_rows + row
        chosen = jnp.where(iota(pick.shape, 1).astype(F32) == target, 1.0, 0.0)
        side = jnp.where(holder >= n_half, 1.0, 0.0)
        return chosen.astype(jnp.bfloat16), start, jnp.where(side == half.astype(F32), 1.0, 0.0)

    def framed(member):
        square = (tok, tok)
        before = jnp.where(iota(square, 1) < iota(square, 0), 1.0, 0.0).astype(jnp.bfloat16)
        wide = jnp.broadcast_to(member, (tok, D_HEAD)).astype(jnp.bfloat16)
        rank = jnp.dot(before, wide, preferred_element_type=F32)[:, 0:1]
        at = jnp.where(rank < keep_rows, rank, float(2 * keep_rows + spill - 1) - rank)
        at = jnp.where(member > 0.0, at, -1.0)
        return jnp.where(iota(square, 1).astype(F32) == at, 1.0, 0.0).astype(jnp.bfloat16)

    @pl.when(is_relay)
    def _():
        for j in range(2):
            chosen, _, member = locate(far_request(lane, j))
            relay_pick[j] = lax.dot_general(
                framed(member), chosen, (((0,), (0,)), ((), ())), preferred_element_type=F32
            ).astype(jnp.bfloat16)

    near, start, member = locate(me)
    pick[...] = near
    far_pick[...] = framed(1.0 - member)
    angle = start * inv_ref[...]
    cosine[...] = jnp.cos(angle)
    sine[...] = jnp.sin(angle) * jnp.where(iota((1, D_HEAD), 1) < D_HEAD // 2, -1.0, 1.0)
    chosen = sel_ref[...].astype(F32)
    matches = jnp.where(iota((tok, sel), 0).astype(F32) + first == chosen, 1.0, 0.0)
    fresh_pick[...] = matches.astype(jnp.bfloat16)
    is_fresh[...] = jnp.broadcast_to(jnp.sum(matches, axis=1, keepdims=True), is_fresh.shape)
    limit[...] = jnp.broadcast_to(column(chosen), limit.shape)

    def gather(c, peer_chip):
        block = kv_all.at[stripe, c]
        return pltpu.make_async_remote_copy(
            src_ref=block, dst_ref=block,
            send_sem=gather_send.at[c, peer_chip], recv_sem=gather_recv.at[c, stripe],
            device_id={"seq": peer_chip * 2 + core}, device_id_type=MESH,
        )

    def arrival(c, source):
        block = kv_all.at[source, c]
        return pltpu.make_async_remote_copy(
            src_ref=block, dst_ref=block,
            send_sem=forward_send.at[c, source // 2], recv_sem=gather_recv.at[c, source],
            device_id={"seq": sibling}, device_id_type=MESH,
        )

    def pair(c):
        block = kv_all.at[stripe, c]
        return pltpu.make_async_remote_copy(
            src_ref=block, dst_ref=block,
            send_sem=pair_send.at[c], recv_sem=gather_recv.at[c, stripe],
            device_id={"seq": sibling}, device_id_type=MESH,
        )

    def kv_store(c, part):
        return pltpu.make_async_copy(
            kv_all.at[stripe, c, :, pl.ds(part * CW, CW)],
            kv_out.at[0, :, part_cols(c, part)],
            kv_sem.at[c, part],
        )

    def out_cols(c):
        width = HPC * GROUPS * D_HEAD
        return pl.ds(pl.multiple_of(c * width, width), width)

    def ov_store(c):
        return pltpu.make_async_copy(ov.at[:, out_cols(c)], attn_out.at[0, :, out_cols(c)], ov_sem.at[c])

    def blend(c):
        for part in range(2):
            cols = part_cols(c, part)
            slots = landing[:, :, cols].reshape(n_half * slot_rows, CW)
            cached = jnp.dot(pick[...], slots, preferred_element_type=F32)
            cached = cached + jnp.dot(
                far_pick[...], far[c, :, part * CW:(part + 1) * CW], preferred_element_type=F32
            )
            fresh = jnp.dot(fresh_pick[...], fresh_ref[0, :, cols], preferred_element_type=F32)
            for i in range(HPC):
                lanes = slice(i * D_HEAD, (i + 1) * D_HEAD)
                x = cached[:, lanes]
                if part == 0:
                    x = x * cosine[...] + pltpu.roll(x, D_HEAD // 2, 1) * sine[...]
                x = jnp.where(is_fresh[...] > 0.0, fresh[:, lanes], x)
                at = part * CW + i * D_HEAD
                kv_all[stripe, c, :, at:at + D_HEAD] = x.astype(jnp.bfloat16)

    scale = math.log2(math.e) / math.sqrt(D_HEAD)
    contract = (((1,), (1,)), ((), ()))

    def attend(c):
        for i in range(HPC):
            base = (c * HPC + i) * GROUPS * D_HEAD
            wide = qv[:, pl.ds(pl.multiple_of(base, GROUPS * D_HEAD), GROUPS * D_HEAD)]
            q = jnp.concatenate(
                [wide[:, g * D_HEAD:(g + 1) * D_HEAD] for g in range(GROUPS)], axis=0
            )
            k_lanes = slice(i * D_HEAD, (i + 1) * D_HEAD)
            v_lanes = slice(CW + i * D_HEAD, CW + (i + 1) * D_HEAD)

            def scores_of(s):
                keys = kv_all[s, c, :, k_lanes]
                return lax.dot_general(q, keys, contract, preferred_element_type=F32) * scale

            scores = scores_of(stripe)
            keep = iota((sel, tok), 1).astype(F32) + first <= limit[:, 0:1]
            keep = jnp.concatenate([jnp.where(keep, 0.0, -1e30)] * GROUPS, axis=0)
            scores = jnp.where(keep < 0.0, -1e30, scores)
            top = jnp.max(scores, axis=1, keepdims=True)
            weights = jnp.exp2(scores - top)
            total = jnp.sum(weights, axis=1, keepdims=True)
            acc = jnp.dot(
                weights.astype(jnp.bfloat16), kv_all[stripe, c, :, v_lanes],
                preferred_element_type=F32,
            )

            def earlier(s, state):
                top, total, acc = state
                scores = scores_of(s)
                raised = jnp.maximum(top, jnp.max(scores, axis=1, keepdims=True))
                fade = jnp.exp2(top - raised)
                weights = jnp.exp2(scores - raised)
                total = total * fade + jnp.sum(weights, axis=1, keepdims=True)
                acc = acc * fade + jnp.dot(
                    weights.astype(jnp.bfloat16), kv_all[s, c, :, v_lanes],
                    preferred_element_type=F32,
                )
                return raised, total, acc

            top, total, acc = lax.fori_loop(0, stripe, earlier, (top, total, acc))
            normed = acc * (1.0 / total)
            live = limit[...] >= 0.0
            for g in range(GROUPS):
                part = jnp.where(live, normed[g * sel:(g + 1) * sel], 0.0)
                ov[:, pl.ds(pl.multiple_of(base + g * D_HEAD, D_HEAD), D_HEAD)] = part.astype(jnp.bfloat16)

    def relay(c):
        for j in range(2):
            for part in range(2):
                for d in range(1, n_half):
                    to_relay(c, (local + d) % n_half, lane, j, part).wait_recv()

        @pl.when(c == 0)
        def _():
            for j in range(2):
                own_relay(j).wait()

        for j in range(2):
            for part in range(2):
                slots = relay_in[j, :, :, part_cols(c, part)].reshape(n_half * slot_rows, CW)
                rows = jnp.dot(relay_pick[j], slots, preferred_element_type=F32)
                cols = slice(part * CW, (part + 1) * CW)
                merged[j, c, :, cols] = rows[:keep_rows].astype(jnp.bfloat16)
                if spill:
                    tail_out[j, c, :, cols] = rows[keep_rows:].astype(jnp.bfloat16)
            if spill:
                relay_tail(c, j).start()

        for j in range(2):
            if spill:
                relay_tail(c, j).wait_recv()
                merged[j, c, keep_rows - spill:] = merged[j, c, keep_rows - spill:] + tail_in[j, c]
            relay_out(c, j).start()

    def step(t, carry):
        @pl.when((t < CHUNKS) & is_relay)
        def _():
            relay(t)

        c = t - LAG

        @pl.when((c >= 0) & (c < CHUNKS))
        def _():
            relay_out(c, 0).wait_recv()
            if spill:
                far_tail(c).start()

        @pl.when(c > 0)
        def _():
            last = c - 1
            for a in range(n_chips - 1):
                @pl.when(a < chip)
                def _():
                    arrival(last, a * 2 + 1 - core).wait_recv()

            @pl.when(core == 1)
            def _():
                arrival(last, chip * 2).wait_recv()

            attend(last)
            ov_store(last).start()

        @pl.when((c >= 0) & (c < CHUNKS))
        def _():
            for d in range(1, n_half):
                for part in range(2):
                    fetch(c, (local + d) % n_half, local, part).wait_recv()

            @pl.when(c == 0)
            def _():
                own_copy.wait()
                q_copy.wait()

            if spill:
                far_tail(c).wait_recv()
            blend(c)
            for b in range(1, n_chips):
                @pl.when(chip < b)
                def _():
                    gather(c, b).start()

            @pl.when(core == 0)
            def _():
                pair(c).start()

            for part in range(2):
                kv_store(c, part).start()

            for a in range(n_chips - 1):
                @pl.when(a < chip)
                def _():
                    arrival(c, a * 2 + core).wait_recv()
                    arrival(c, a * 2 + core).start()

        return carry

    lax.fori_loop(0, CHUNKS + LAG + 1, step, 0)

    def drain(c, carry):
        each_to_relay(c, lambda copy: copy.wait_send())
        for d in range(1, n_half):
            for part in range(2):
                fetch(c, local, (local + d) % n_half, part).wait_send()

        @pl.when(is_relay)
        def _():
            for j in range(2):
                if spill:
                    relay_tail(c, j).wait_send()
                relay_out(c, j).wait_send()

        if spill:
            far_tail(c).wait_send()

        for b in range(1, n_chips):
            @pl.when(chip < b)
            def _():
                gather(c, b).wait_send()

        @pl.when(core == 0)
        def _():
            pair(c).wait_send()

        for a in range(n_chips - 1):
            @pl.when(a < chip)
            def _():
                arrival(c, a * 2 + core).wait_send()

        for part in range(2):
            kv_store(c, part).wait()
        ov_store(c).wait()
        return carry

    lax.fori_loop(0, CHUNKS, drain, 0)


def on_device(n_store, n_seq, store_kv, span_len, span_shard, q_sel, fresh_kv, sel_pos):
    slot_rows = store_kv.shape[1]
    tok = 256
    sel = sel_pos.shape[1]
    half = np.arange(D_HEAD // 2, dtype=np.float64) * 2.0 / D_HEAD
    inverse = np.power(ROPE_BASE, -np.concatenate([half, half]))[None].astype(np.float32)
    hbm = pl.BlockSpec(memory_space=pl.ANY)
    vmem = pl.BlockSpec(memory_space=pltpu.VMEM)
    dma = pltpu.SemaphoreType.DMA
    bf16 = jnp.bfloat16
    n_chips = n_seq // 2
    n_half = n_store // 2
    keep_rows = frame_rows(n_store, slot_rows, tok)
    spill = tok - keep_rows
    return pl.pallas_call(
        functools.partial(kernel, n_store, n_seq),
        out_shape=(
            jax.ShapeDtypeStruct((1, tok, 2 * KV_WIDTH), bf16),
            jax.ShapeDtypeStruct((1, sel, HEADS * D_HEAD), bf16),
        ),
        in_specs=[hbm, vmem, vmem, vmem, hbm, vmem, vmem],
        out_specs=(hbm, hbm),
        scratch_shapes=[
            pltpu.VMEM((n_half, slot_rows, 2 * KV_WIDTH), bf16),
            pltpu.VMEM((2, n_half, slot_rows, 2 * KV_WIDTH), bf16),
            pltpu.VMEM((2, CHUNKS, keep_rows, 2 * CW), bf16),
            pltpu.VMEM((CHUNKS, tok, 2 * CW), bf16),
            pltpu.VMEM((n_seq, CHUNKS, tok, 2 * CW), bf16),
            pltpu.VMEM((sel, HEADS * D_HEAD), bf16),
            pltpu.VMEM((sel, HEADS * D_HEAD), bf16),
            pltpu.VMEM((tok, n_half * slot_rows), bf16),
            pltpu.VMEM((tok, tok), bf16),
            pltpu.VMEM((2, tok, n_half * slot_rows), bf16),
            pltpu.VMEM((tok, sel), bf16),
            pltpu.VMEM((2, CHUNKS, spill, 2 * CW), bf16),
            pltpu.VMEM((2, CHUNKS, spill, 2 * CW), bf16),
            pltpu.VMEM((tok, D_HEAD), F32),
            pltpu.VMEM((tok, D_HEAD), F32),
            pltpu.VMEM((tok, D_HEAD), F32),
            pltpu.VMEM((sel, D_HEAD), F32),
            dma((CHUNKS, n_half, 2)),
            dma((CHUNKS, n_half, 2)),
            dma((CHUNKS, 2, n_store // 4, 2)),
            dma((CHUNKS, 2, n_half, 2)),
            dma((CHUNKS, 2)),
            dma((CHUNKS,)),
            dma((CHUNKS, 2)),
            dma((CHUNKS, 2)),
            dma((CHUNKS,)),
            dma((CHUNKS,)),
            dma((3,)),
            dma(()),
            dma((CHUNKS, n_chips)),
            dma((CHUNKS, n_seq)),
            dma((CHUNKS, n_chips)),
            dma((CHUNKS,)),
            dma((CHUNKS, 2)),
            dma((CHUNKS,)),
        ],
        compiler_params=pltpu.CompilerParams(
            collective_id=0, has_side_effects=True, vmem_limit_bytes=60 * 1024 * 1024
        ),
    )(store_kv, span_len, span_shard, jnp.asarray(inverse), q_sel, fresh_kv, sel_pos)


def solution(mesh):
    n_store, n_seq = mesh.shape["store"], mesh.shape["seq"]
    return jax.shard_map(
        functools.partial(on_device, n_store, n_seq),
        mesh=mesh,
        in_specs=(
            P("store", "seq", None),
            P(),
            P(),
            P("store", "seq", None),
            P("store", "seq", None),
            P("store", "seq"),
        ),
        out_specs=(P("store", "seq", None), P("store", "seq", None)),
        check_vma=False,
    )
```

```python
import functools
import math

import jax
import jax.numpy as jnp
import numpy as np
from jax import lax
from jax.experimental import pallas as pl
from jax.experimental.pallas import tpu as pltpu
from jax.sharding import PartitionSpec as P

HEADS = 64
KV_HEADS = 8
D_HEAD = 128
GROUPS = HEADS // KV_HEADS
KV_WIDTH = KV_HEADS * D_HEAD
ROPE_BASE = 500000.0
CHUNKS = KV_HEADS
LAG = 2
LEAD = 2
SHORTEST, LONGEST = 37, 80
CW = D_HEAD
F32 = jnp.float32
MESH = pl.DeviceIdType.MESH


def iota(shape, axis):
    return lax.broadcasted_iota(jnp.int32, shape, axis)


def own_row(ref, row):
    table = ref[...].astype(F32)
    return jnp.sum(jnp.where(iota(table.shape, 0) == row, table, 0.0), axis=0, keepdims=True)


def column(row):
    n = row.shape[1]
    square = (n, n)
    return jnp.sum(jnp.where(iota(square, 0) == iota(square, 1), row, 0.0), axis=1, keepdims=True)


def frame_rows(n_store, slot_rows, tok):
    half = n_store // 2
    shortest = slot_rows * SHORTEST // LONGEST
    window = 2 * tok
    most, m = 0, 0
    while window > m * half * shortest:
        most = max(most, min((m + 1) * half * slot_rows, window - m * half * shortest))
        m += 1
    return min(tok, -(-most // 32) * 16)


def kernel(
    n_store, n_seq,
    store_ref, len_hbm, shard_hbm, inv_hbm, q_ref, fresh_hbm, sel_hbm,
    kv_out, attn_out,
    len_ref, shard_ref, inv_ref, fresh_ref, sel_ref,
    landing, relay_in, merged, far, kv_all, qv, scores, pick, far_pick, relay_pick, fresh_pick, tail_out, tail_in, is_fresh, cosine, sine, limit,
    fetch_send, fetch_recv, relay_send, relay_recv, merged_send, far_recv,
    tail_send, tail_recv, spill_send, spill_recv,
    own_sem, q_sem, gather_send, direct_recv, sibling_recv, pair_recv,
    forward_send, pair_send, load_sem,
):
    me = lax.axis_index("store")
    stripe = lax.axis_index("seq")
    slot_rows = store_ref.shape[1]
    tok = kv_out.shape[1]
    sel = sel_ref.shape[1]
    keep_rows = merged.shape[2]
    spill = tok - keep_rows
    n_chips = n_seq // 2
    chip = stripe // 2
    core = stripe % 2
    sibling = chip * 2 + (1 - core)
    n_half = n_store // 2
    ny = n_store // 4
    half = me // n_half
    local = me % n_half
    lane = me % ny
    relay_row = 1 + half
    is_relay = me // ny == relay_row

    barrier = pltpu.get_barrier_semaphore()
    for d in range(1, n_half):
        peer = half * n_half + (local + d) % n_half
        pl.semaphore_signal(barrier, inc=1, device_id={"store": peer}, device_id_type=MESH)
    pl.semaphore_signal(barrier, inc=1, device_id={"store": (2 - half) * ny + lane}, device_id_type=MESH)
    for d in range(1, n_seq):
        pl.semaphore_signal(barrier, inc=1, device_id={"seq": (stripe + d) % n_seq}, device_id_type=MESH)

    loads = [
        pltpu.make_async_copy(src, dst, load_sem.at[i])
        for i, (src, dst) in enumerate([
            (len_hbm, len_ref), (shard_hbm, shard_ref), (inv_hbm, inv_ref), (sel_hbm, sel_ref), (fresh_hbm, fresh_ref),
        ])
    ]
    for load in loads:
        load.start()

    peers = n_half + n_seq - 2

    @pl.when(is_relay)
    def _():
        pl.semaphore_wait(barrier, peers + 2)

    @pl.when(jnp.logical_not(is_relay))
    def _():
        pl.semaphore_wait(barrier, peers)

    def part_cols(c, part):
        return pl.ds(pl.multiple_of(part * KV_WIDTH + c * CW, CW), CW)

    def fetch(c, src, dst, part):
        cols = part_cols(c, part)
        return pltpu.make_async_remote_copy(
            src_ref=store_ref.at[half * n_half + dst, :, cols],
            dst_ref=landing.at[src, :, cols],
            send_sem=fetch_send,
            recv_sem=fetch_recv.at[c, part],
            device_id={"store": half * n_half + dst},
            device_id_type=MESH,
        )

    def far_request(y, j):
        return ((1 - half) * 2 + j) * ny + y

    def to_relay(c, src, y, j, part):
        cols = part_cols(c, part)
        return pltpu.make_async_remote_copy(
            src_ref=store_ref.at[far_request(y, j), :, cols],
            dst_ref=relay_in.at[j, src, :, cols],
            send_sem=relay_send,
            recv_sem=relay_recv.at[c, part],
            device_id={"store": relay_row * ny + y},
            device_id_type=MESH,
        )

    def relay_out(c, j):
        return pltpu.make_async_remote_copy(
            src_ref=merged.at[j, c],
            dst_ref=far.at[c, pl.ds(0, keep_rows)],
            send_sem=merged_send,
            recv_sem=far_recv.at[c],
            device_id={"store": far_request(lane, j)},
            device_id_type=MESH,
        )

    def relay_tail(c, j):
        return pltpu.make_async_remote_copy(
            src_ref=tail_out.at[j, c],
            dst_ref=tail_in.at[j, c],
            send_sem=tail_send,
            recv_sem=tail_recv.at[c],
            device_id={"seq": sibling},
            device_id_type=MESH,
        )

    def far_tail(c):
        return pltpu.make_async_remote_copy(
            src_ref=far.at[c, pl.ds(keep_rows - spill, spill)],
            dst_ref=far.at[c, pl.ds(keep_rows, spill)],
            send_sem=spill_send,
            recv_sem=spill_recv.at[c],
            device_id={"seq": sibling},
            device_id_type=MESH,
        )

    own_copy = pltpu.make_async_copy(store_ref.at[me], landing.at[local], own_sem.at[0])
    q_copy = pltpu.make_async_copy(q_ref.at[0], qv, q_sem)

    def own_relay(j):
        return pltpu.make_async_copy(
            store_ref.at[far_request(lane, j)], relay_in.at[j, local], own_sem.at[1 + j]
        )

    def each_to_relay(c, act):
        for j in range(2):
            for part in range(2):
                @pl.when(jnp.logical_not(is_relay))
                def _():
                    act(to_relay(c, local, lane, j, part))

                for d in range(1, ny):
                    act(to_relay(c, local, (lane + d) % ny, j, part))

    def issue(t, carry):
        @pl.when(t < CHUNKS)
        def _():
            each_to_relay(t, lambda copy: copy.start())

        @pl.when(t >= LEAD)
        def _():
            for d in range(1, n_half):
                for part in range(2):
                    fetch(t - LEAD, local, (local + d) % n_half, part).start()

        return carry

    lax.fori_loop(0, CHUNKS + LEAD, issue, 0)
    own_copy.start()

    @pl.when(is_relay)
    def _():
        for j in range(2):
            own_relay(j).start()

    q_copy.start()

    for load in loads:
        load.wait()

    first = (stripe * tok).astype(F32)
    n_span = len_ref.shape[1]

    def locate(request):
        lengths = own_row(len_ref, request)
        square = (n_span, n_span)
        starts = jnp.sum(
            jnp.where(iota(square, 0) < iota(square, 1), column(lengths), 0.0), axis=0, keepdims=True
        )
        shards = column(own_row(shard_ref, request))
        spread = (n_store, n_span)
        holders = jnp.sum(
            jnp.where(iota(spread, 1) % n_store == iota(spread, 0), shards, 0.0), axis=0, keepdims=True
        )
        grid = (tok, n_span)
        position = iota(grid, 0).astype(F32) + first
        which = jnp.sum(jnp.where(position >= starts, 1.0, 0.0), axis=1, keepdims=True) - 1.0
        picked = iota(grid, 1).astype(F32) == which
        holder = jnp.sum(jnp.where(picked, holders, 0.0), axis=1, keepdims=True)
        start = jnp.sum(jnp.where(picked, starts, 0.0), axis=1, keepdims=True)
        row = iota((tok, 1), 0).astype(F32) + first - jnp.maximum(start, first)
        target = (holder - (half * n_half).astype(F32)) * slot_rows + row
        chosen = jnp.where(iota(pick.shape, 1).astype(F32) == target, 1.0, 0.0)
        side = jnp.where(holder >= n_half, 1.0, 0.0)
        return chosen.astype(jnp.bfloat16), start, jnp.where(side == half.astype(F32), 1.0, 0.0)

    def framed(member):
        square = (tok, tok)
        before = jnp.where(iota(square, 1) < iota(square, 0), 1.0, 0.0).astype(jnp.bfloat16)
        wide = jnp.broadcast_to(member, (tok, D_HEAD)).astype(jnp.bfloat16)
        rank = jnp.dot(before, wide, preferred_element_type=F32)[:, 0:1]
        at = jnp.where(rank < keep_rows, rank, float(2 * keep_rows + spill - 1) - rank)
        at = jnp.where(member > 0.0, at, -1.0)
        return jnp.where(iota(square, 1).astype(F32) == at, 1.0, 0.0).astype(jnp.bfloat16)

    @pl.when(is_relay)
    def _():
        for j in range(2):
            chosen, _, member = locate(far_request(lane, j))
            relay_pick[j] = lax.dot_general(
                framed(member), chosen, (((0,), (0,)), ((), ())), preferred_element_type=F32
            ).astype(jnp.bfloat16)

    near, start, member = locate(me)
    pick[...] = near
    far_pick[...] = framed(1.0 - member)
    angle = start * inv_ref[...]
    cosine[...] = jnp.cos(angle)
    sine[...] = jnp.sin(angle) * jnp.where(iota((1, D_HEAD), 1) < D_HEAD // 2, -1.0, 1.0)
    chosen = sel_ref[...].astype(F32)
    matches = jnp.where(iota((tok, sel), 0).astype(F32) + first == chosen, 1.0, 0.0)
    fresh_pick[...] = matches.astype(jnp.bfloat16)
    is_fresh[...] = jnp.broadcast_to(jnp.sum(matches, axis=1, keepdims=True), is_fresh.shape)
    limit[...] = jnp.broadcast_to(column(chosen), limit.shape)

    def gather(c, peer_chip, part):
        block = kv_all.at[stripe, c, part]
        return pltpu.make_async_remote_copy(
            src_ref=block, dst_ref=block,
            send_sem=gather_send.at[peer_chip], recv_sem=direct_recv.at[c, chip, part],
            device_id={"seq": peer_chip * 2 + core}, device_id_type=MESH,
        )

    def direct(c, a, part):
        block = kv_all.at[a * 2 + core, c, part]
        return pltpu.make_async_copy(block, block, direct_recv.at[c, a, part])

    def passed_on(c, a, part):
        block = kv_all.at[a * 2 + core, c, part]
        return pltpu.make_async_remote_copy(
            src_ref=block, dst_ref=block,
            send_sem=forward_send.at[a], recv_sem=sibling_recv.at[c, a, part],
            device_id={"seq": sibling}, device_id_type=MESH,
        )

    def pair(c, part):
        block = kv_all.at[stripe, c, part]
        return pltpu.make_async_remote_copy(
            src_ref=block, dst_ref=block,
            send_sem=pair_send, recv_sem=pair_recv.at[c, part],
            device_id={"seq": sibling}, device_id_type=MESH,
        )

    def settle(ref, sem):
        pltpu.make_async_copy(ref, ref, sem).wait()

    def blend(c, part):
        cols = part_cols(c, part)
        slots = landing[:, :, cols].reshape(n_half * slot_rows, CW)
        x = jnp.dot(pick[...], slots, preferred_element_type=F32)
        x = x + jnp.dot(far_pick[...], far[c, :, part * CW:(part + 1) * CW], preferred_element_type=F32)
        fresh = jnp.dot(fresh_pick[...], fresh_ref[0, :, cols], preferred_element_type=F32)
        if part == 0:
            x = x * cosine[...] + pltpu.roll(x, D_HEAD // 2, 1) * sine[...]
        x = jnp.where(is_fresh[...] > 0.0, fresh, x)
        x = x.astype(jnp.bfloat16)
        kv_all[stripe, c, part] = x
        kv_out[0, :, cols] = x

    scale = math.log2(math.e) / math.sqrt(D_HEAD)
    contract = (((1,), (1,)), ((), ()))

    def forward(c, part):
        for a in range(n_chips - 1):
            @pl.when(a < chip)
            def _():
                direct(c, a, part).wait()
                passed_on(c, a, part).start()

    def await_sibling(c, part):
        for a in range(n_chips - 1):
            @pl.when(a < chip)
            def _():
                settle(kv_all.at[a * 2 + 1 - core, c, part], sibling_recv.at[c, a, part])

        @pl.when(core == 1)
        def _():
            settle(kv_all.at[chip * 2, c, part], pair_recv.at[c, part])

    def peak_of(x):
        top = x[:, :D_HEAD]
        for i in range(1, tok // D_HEAD):
            top = jnp.maximum(top, x[:, i * D_HEAD:(i + 1) * D_HEAD])
        return top

    def attend(c):
        base = c * GROUPS * D_HEAD
        wide = qv[:, pl.ds(pl.multiple_of(base, GROUPS * D_HEAD), GROUPS * D_HEAD)]
        q = jnp.concatenate([wide[:, g * D_HEAD:(g + 1) * D_HEAD] for g in range(GROUPS)], axis=0)

        def scores_of(s):
            return lax.dot_general(q, kv_all[s, c, 0], contract, preferred_element_type=F32)

        own = scores_of(stripe)
        keep = iota((sel, tok), 1).astype(F32) + first <= limit[:, 0:1]
        keep = jnp.concatenate([jnp.where(keep, 0.0, -1e30)] * GROUPS, axis=0)
        own = jnp.where(keep < 0.0, -1e30, own)
        scores[stripe] = own
        await_sibling(c, 0)

        def score(s, top):
            x = scores_of(s)
            scores[s] = x
            return jnp.maximum(top, peak_of(x))

        top = lax.fori_loop(0, stripe, score, peak_of(own))
        top = jnp.max(top, axis=1, keepdims=True) * scale
        forward(c, 1)
        ones = jnp.ones((tok, D_HEAD), jnp.bfloat16)

        def weighted(s):
            weights = jnp.exp2(scores[s] * scale - top).astype(jnp.bfloat16)
            return jnp.dot(
                weights, jnp.concatenate([kv_all[s, c, 1], ones], axis=1), preferred_element_type=F32
            )

        acc = weighted(stripe)
        await_sibling(c, 1)
        acc = lax.fori_loop(0, stripe, lambda s, acc: acc + weighted(s), acc)
        normed = acc[:, :D_HEAD] * (1.0 / acc[:, D_HEAD:])
        live = limit[...] >= 0.0
        for g in range(GROUPS):
            part = jnp.where(live, normed[g * sel:(g + 1) * sel], 0.0)
            attn_out[0, :, pl.ds(pl.multiple_of(base + g * D_HEAD, D_HEAD), D_HEAD)] = part.astype(jnp.bfloat16)

    def relay(c):
        for part in range(2):
            settle(relay_in.at[:, pl.ds(0, n_half - 1), :, part_cols(c, part)], relay_recv.at[c, part])

        @pl.when(c == 0)
        def _():
            for j in range(2):
                own_relay(j).wait()

        for j in range(2):
            for part in range(2):
                slots = relay_in[j, :, :, part_cols(c, part)].reshape(n_half * slot_rows, CW)
                rows = jnp.dot(relay_pick[j], slots, preferred_element_type=F32)
                cols = slice(part * CW, (part + 1) * CW)
                merged[j, c, :, cols] = rows[:keep_rows].astype(jnp.bfloat16)
                if spill:
                    tail_out[j, c, :, cols] = rows[keep_rows:].astype(jnp.bfloat16)
            if spill:
                relay_tail(c, j).start()

        if spill:
            settle(tail_in.at[:, c], tail_recv.at[c])
        for j in range(2):
            if spill:
                merged[j, c, keep_rows - spill:] = merged[j, c, keep_rows - spill:] + tail_in[j, c]
            relay_out(c, j).start()

    def step(t, carry):
        @pl.when((t < CHUNKS) & is_relay)
        def _():
            relay(t)

        c = t - LAG

        @pl.when(c > 0)
        def _():
            forward(c - 1, 0)

        @pl.when((c >= 0) & (c < CHUNKS))
        def _():
            relay_out(c, 0).wait_recv()
            if spill:
                far_tail(c).start()

        @pl.when(c > 0)
        def _():
            attend(c - 1)

        @pl.when((c >= 0) & (c < CHUNKS))
        def _():
            @pl.when(c == 0)
            def _():
                own_copy.wait()
                q_copy.wait()

            if spill:
                far_tail(c).wait_recv()

            for part in range(2):
                settle(landing.at[pl.ds(0, n_half - 1), :, part_cols(c, part)], fetch_recv.at[c, part])
                blend(c, part)
                for b in range(1, n_chips):
                    @pl.when(chip < b)
                    def _():
                        gather(c, b, part).start()

                @pl.when(core == 0)
                def _():
                    pair(c, part).start()


        return carry

    lax.fori_loop(0, CHUNKS + LAG + 1, step, 0)

    settle(landing.at[pl.ds(0, n_half - 1)], fetch_send)

    @pl.when(is_relay)
    def _():
        settle(relay_in.at[:, pl.ds(0, ny - 1)], relay_send)
        settle(merged, merged_send)
        if spill:
            settle(tail_out, tail_send)

    @pl.when(jnp.logical_not(is_relay))
    def _():
        settle(relay_in.at[:, pl.ds(0, ny)], relay_send)

    if spill:
        settle(tail_in.at[0], spill_send)

    for b in range(1, n_chips):
        @pl.when(chip < b)
        def _():
            settle(kv_all.at[0], gather_send.at[b])

    for a in range(n_chips - 1):
        @pl.when(a < chip)
        def _():
            settle(kv_all.at[0], forward_send.at[a])

    @pl.when(core == 0)
    def _():
        settle(kv_all.at[0], pair_send)


def on_device(n_store, n_seq, store_kv, span_len, span_shard, q_sel, fresh_kv, sel_pos):
    slot_rows = store_kv.shape[1]
    tok = 256
    sel = sel_pos.shape[1]
    half = np.arange(D_HEAD // 2, dtype=np.float64) * 2.0 / D_HEAD
    inverse = np.power(ROPE_BASE, -np.concatenate([half, half]))[None].astype(np.float32)
    hbm = pl.BlockSpec(memory_space=pl.ANY)
    dma = pltpu.SemaphoreType.DMA
    bf16 = jnp.bfloat16
    n_chips = n_seq // 2
    n_half = n_store // 2
    keep_rows = frame_rows(n_store, slot_rows, tok)
    spill = tok - keep_rows
    return pl.pallas_call(
        functools.partial(kernel, n_store, n_seq),
        out_shape=(
            pltpu.VMEM((1, tok, 2 * KV_WIDTH), bf16),
            pltpu.VMEM((1, sel, HEADS * D_HEAD), bf16),
        ),
        in_specs=[hbm] * 7,
        out_specs=(pl.BlockSpec(memory_space=pltpu.VMEM),) * 2,
        scratch_shapes=[
            pltpu.VMEM(span_len.shape, jnp.int32),
            pltpu.VMEM(span_shard.shape, jnp.int32),
            pltpu.VMEM(inverse.shape, F32),
            pltpu.VMEM(fresh_kv.shape, bf16),
            pltpu.VMEM(sel_pos.shape, jnp.int32),
            pltpu.VMEM((n_half, slot_rows, 2 * KV_WIDTH), bf16),
            pltpu.VMEM((2, n_half, slot_rows, 2 * KV_WIDTH), bf16),
            pltpu.VMEM((2, CHUNKS, keep_rows, 2 * CW), bf16),
            pltpu.VMEM((CHUNKS, tok, 2 * CW), bf16),
            pltpu.VMEM((n_seq, CHUNKS, 2, tok, CW), bf16),
            pltpu.VMEM((sel, HEADS * D_HEAD), bf16),
            pltpu.VMEM((n_seq, GROUPS * sel, tok), F32),
            pltpu.VMEM((tok, n_half * slot_rows), bf16),
            pltpu.VMEM((tok, tok), bf16),
            pltpu.VMEM((2, tok, n_half * slot_rows), bf16),
            pltpu.VMEM((tok, sel), bf16),
            pltpu.VMEM((2, CHUNKS, spill, 2 * CW), bf16),
            pltpu.VMEM((2, CHUNKS, spill, 2 * CW), bf16),
            pltpu.VMEM((tok, D_HEAD), F32),
            pltpu.VMEM((tok, D_HEAD), F32),
            pltpu.VMEM((tok, D_HEAD), F32),
            pltpu.VMEM((sel, D_HEAD), F32),
            dma(()),
            dma((CHUNKS, 2)),
            dma(()),
            dma((CHUNKS, 2)),
            dma(()),
            dma((CHUNKS,)),
            dma(()),
            dma((CHUNKS,)),
            dma(()),
            dma((CHUNKS,)),
            dma((3,)),
            dma(()),
            dma((n_chips,)),
            dma((CHUNKS, n_chips - 1, 2)),
            dma((CHUNKS, n_chips - 1, 2)),
            dma((CHUNKS, 2)),
            dma((n_chips,)),
            dma(()),
            dma((5,)),
        ],
        compiler_params=pltpu.CompilerParams(
            collective_id=0, has_side_effects=True, vmem_limit_bytes=60 * 1024 * 1024
        ),
    )(store_kv, span_len, span_shard, jnp.asarray(inverse), q_sel, fresh_kv, sel_pos)


def solution(mesh):
    n_store, n_seq = mesh.shape["store"], mesh.shape["seq"]
    return jax.shard_map(
        functools.partial(on_device, n_store, n_seq),
        mesh=mesh,
        in_specs=(
            P("store", "seq", None),
            P(),
            P(),
            P("store", "seq", None),
            P("store", "seq", None),
            P("store", "seq"),
        ),
        out_specs=(P("store", "seq", None), P("store", "seq", None)),
        check_vma=False,
    )
```

```python
import functools
import math

import jax
import jax.numpy as jnp
import numpy as np
from jax import lax
from jax.experimental import pallas as pl
from jax.experimental.pallas import tpu as pltpu
from jax.sharding import PartitionSpec as P

HEADS = 64
KV_HEADS = 8
D_HEAD = 128
GROUPS = HEADS // KV_HEADS
KV_WIDTH = KV_HEADS * D_HEAD
ROPE_BASE = 500000.0
CHUNKS = KV_HEADS
LEAD = 3
BURST = 5
SPAN = 4
SHORTEST, LONGEST = 37, 80
CW = D_HEAD
F32 = jnp.float32
MESH = pl.DeviceIdType.MESH


def iota(shape, axis):
    return lax.broadcasted_iota(jnp.int32, shape, axis)


def own_row(ref, row):
    table = ref[...].astype(F32)
    return jnp.sum(jnp.where(iota(table.shape, 0) == row, table, 0.0), axis=0, keepdims=True)


def column(row):
    n = row.shape[1]
    square = (n, n)
    return jnp.sum(jnp.where(iota(square, 0) == iota(square, 1), row, 0.0), axis=1, keepdims=True)


def frame_rows(n_store, slot_rows, tok):
    half = n_store // 2
    shortest = slot_rows * SHORTEST // LONGEST
    window = 2 * tok
    most, m = 0, 0
    while window > m * half * shortest:
        most = max(most, min((m + 1) * half * slot_rows, window - m * half * shortest))
        m += 1
    return min(tok, -(-most // 32) * 16)


def kernel(
    n_store, n_seq,
    store_ref, len_hbm, shard_hbm, inv_hbm, q_ref, fresh_hbm, sel_hbm,
    kv_out, attn_out,
    len_ref, shard_ref, inv_ref, fresh_ref, sel_ref,
    landing, relay_in, merged, far, kv_all, qv, scores, pick, far_pick, relay_pick, fresh_pick, tail_out, tail_in, is_fresh, cosine, sine, limit,
    fetch_send, fetch_recv, relay_send, relay_recv, merged_send, far_recv,
    tail_send, tail_recv, spill_send, spill_recv,
    own_sem, q_sem, gather_send, direct_recv, sibling_recv, pair_recv,
    forward_send, pair_send, load_sem,
):
    me = lax.axis_index("store")
    stripe = lax.axis_index("seq")
    slot_rows = store_ref.shape[1]
    tok = kv_out.shape[1]
    sel = sel_ref.shape[1]
    keep_rows = merged.shape[2]
    spill = tok - keep_rows
    n_chips = n_seq // 2
    chip = stripe // 2
    core = stripe % 2
    sibling = chip * 2 + (1 - core)
    n_half = n_store // 2
    ny = n_store // 4
    half = me // n_half
    local = me % n_half
    lane = me % ny
    relay_row = 1 + half
    is_relay = me // ny == relay_row

    barrier = pltpu.get_barrier_semaphore()
    for d in range(1, n_half):
        peer = half * n_half + (local + d) % n_half
        pl.semaphore_signal(barrier, inc=1, device_id={"store": peer}, device_id_type=MESH)
    pl.semaphore_signal(barrier, inc=1, device_id={"store": (2 - half) * ny + lane}, device_id_type=MESH)
    for d in range(1, n_seq):
        pl.semaphore_signal(barrier, inc=1, device_id={"seq": (stripe + d) % n_seq}, device_id_type=MESH)

    loads = [
        pltpu.make_async_copy(src, dst, load_sem.at[i])
        for i, (src, dst) in enumerate([
            (len_hbm, len_ref), (shard_hbm, shard_ref), (inv_hbm, inv_ref), (sel_hbm, sel_ref), (fresh_hbm, fresh_ref),
        ])
    ]
    for load in loads:
        load.start()

    peers = n_half + n_seq - 2

    @pl.when(is_relay)
    def _():
        pl.semaphore_wait(barrier, peers + 2)

    @pl.when(jnp.logical_not(is_relay))
    def _():
        pl.semaphore_wait(barrier, peers)

    def part_cols(c, part):
        return pl.ds(pl.multiple_of(part * KV_WIDTH + c * CW, CW), CW)

    def fetch(c, src, dst, part):
        cols = part_cols(c, part)
        return pltpu.make_async_remote_copy(
            src_ref=store_ref.at[half * n_half + dst, :, cols],
            dst_ref=landing.at[src, :, cols],
            send_sem=fetch_send,
            recv_sem=fetch_recv.at[c, part],
            device_id={"store": half * n_half + dst},
            device_id_type=MESH,
        )

    def far_request(y, j):
        return ((1 - half) * 2 + j) * ny + y

    def to_relay(c, src, y, j, part):
        cols = part_cols(c, part)
        return pltpu.make_async_remote_copy(
            src_ref=store_ref.at[far_request(y, j), :, cols],
            dst_ref=relay_in.at[j, src, :, cols],
            send_sem=relay_send,
            recv_sem=relay_recv.at[c, part],
            device_id={"store": relay_row * ny + y},
            device_id_type=MESH,
        )

    def relay_out(c, j):
        return pltpu.make_async_remote_copy(
            src_ref=merged.at[j, c],
            dst_ref=far.at[c, pl.ds(0, keep_rows)],
            send_sem=merged_send,
            recv_sem=far_recv.at[c],
            device_id={"store": far_request(lane, j)},
            device_id_type=MESH,
        )

    def relay_tail(c, j):
        return pltpu.make_async_remote_copy(
            src_ref=tail_out.at[j, c],
            dst_ref=tail_in.at[j, c],
            send_sem=tail_send,
            recv_sem=tail_recv.at[c],
            device_id={"seq": sibling},
            device_id_type=MESH,
        )

    def far_tail(c):
        return pltpu.make_async_remote_copy(
            src_ref=far.at[c, pl.ds(keep_rows - spill, spill)],
            dst_ref=far.at[c, pl.ds(keep_rows, spill)],
            send_sem=spill_send,
            recv_sem=spill_recv.at[c],
            device_id={"seq": sibling},
            device_id_type=MESH,
        )

    own_copy = pltpu.make_async_copy(store_ref.at[me], landing.at[local], own_sem.at[0])
    q_copy = pltpu.make_async_copy(q_ref.at[0], qv, q_sem)

    def own_relay(j):
        return pltpu.make_async_copy(
            store_ref.at[far_request(lane, j)], relay_in.at[j, local], own_sem.at[1 + j]
        )

    def each_to_relay(c, act):
        for j in range(2):
            for part in range(2):
                @pl.when(jnp.logical_not(is_relay))
                def _():
                    act(to_relay(c, local, lane, j, part))

                for d in range(1, ny):
                    act(to_relay(c, local, (lane + d) % ny, j, part))

    def relayed(c):
        return jnp.where(c < 0, 0, jnp.where(c < BURST, jnp.minimum(c + LEAD, CHUNKS), CHUNKS))

    def issue(c, carry):
        def feed(r, carry):
            each_to_relay(r, lambda copy: copy.start())
            return carry

        lax.fori_loop(relayed(c - 1), relayed(c), feed, 0)
        for d in range(1, n_half):
            for part in range(2):
                fetch(c, local, (local + d) % n_half, part).start()
        return carry

    lax.fori_loop(0, CHUNKS, issue, 0)
    own_copy.start()

    @pl.when(is_relay)
    def _():
        for j in range(2):
            own_relay(j).start()

    q_copy.start()

    for load in loads:
        load.wait()

    first = (stripe * tok).astype(F32)
    n_span = len_ref.shape[1]

    def locate(request):
        lengths = own_row(len_ref, request)
        square = (n_span, n_span)
        starts = jnp.sum(
            jnp.where(iota(square, 0) < iota(square, 1), column(lengths), 0.0), axis=0, keepdims=True
        )
        shards = column(own_row(shard_ref, request))
        spread = (n_store, n_span)
        holders = jnp.sum(
            jnp.where(iota(spread, 1) % n_store == iota(spread, 0), shards, 0.0), axis=0, keepdims=True
        )
        grid = (tok, n_span)
        position = iota(grid, 0).astype(F32) + first
        which = jnp.sum(jnp.where(position >= starts, 1.0, 0.0), axis=1, keepdims=True) - 1.0
        picked = iota(grid, 1).astype(F32) == which
        holder = jnp.sum(jnp.where(picked, holders, 0.0), axis=1, keepdims=True)
        start = jnp.sum(jnp.where(picked, starts, 0.0), axis=1, keepdims=True)
        row = iota((tok, 1), 0).astype(F32) + first - jnp.maximum(start, first)
        target = (holder - (half * n_half).astype(F32)) * slot_rows + row
        chosen = jnp.where(iota(pick.shape, 1).astype(F32) == target, 1.0, 0.0)
        side = jnp.where(holder >= n_half, 1.0, 0.0)
        return chosen.astype(jnp.bfloat16), start, jnp.where(side == half.astype(F32), 1.0, 0.0)

    def framed(member):
        square = (tok, tok)
        before = jnp.where(iota(square, 1) < iota(square, 0), 1.0, 0.0).astype(jnp.bfloat16)
        wide = jnp.broadcast_to(member, (tok, D_HEAD)).astype(jnp.bfloat16)
        rank = jnp.dot(before, wide, preferred_element_type=F32)[:, 0:1]
        at = jnp.where(rank < keep_rows, rank, float(2 * keep_rows + spill - 1) - rank)
        at = jnp.where(member > 0.0, at, -1.0)
        return jnp.where(iota(square, 1).astype(F32) == at, 1.0, 0.0).astype(jnp.bfloat16)

    @pl.when(is_relay)
    def _():
        for j in range(2):
            chosen, _, member = locate(far_request(lane, j))
            relay_pick[j] = lax.dot_general(
                framed(member), chosen, (((0,), (0,)), ((), ())), preferred_element_type=F32
            ).astype(jnp.bfloat16)

    near, start, member = locate(me)
    pick[...] = near
    far_pick[...] = framed(1.0 - member)
    angle = start * inv_ref[...]
    cosine[...] = jnp.cos(angle)
    sine[...] = jnp.sin(angle) * jnp.where(iota((1, D_HEAD), 1) < D_HEAD // 2, -1.0, 1.0)
    chosen = sel_ref[...].astype(F32)
    matches = jnp.where(iota((tok, sel), 0).astype(F32) + first == chosen, 1.0, 0.0)
    fresh_pick[...] = matches.astype(jnp.bfloat16)
    is_fresh[...] = jnp.broadcast_to(jnp.sum(matches, axis=1, keepdims=True), is_fresh.shape)
    limit[...] = jnp.broadcast_to(column(chosen), limit.shape)

    def gather(c, peer_chip, part):
        block = kv_all.at[stripe, c, part]
        return pltpu.make_async_remote_copy(
            src_ref=block, dst_ref=block,
            send_sem=gather_send.at[peer_chip], recv_sem=direct_recv.at[c, chip, part],
            device_id={"seq": peer_chip * 2 + core}, device_id_type=MESH,
        )

    def direct(c, a, part):
        block = kv_all.at[a * 2 + core, c, part]
        return pltpu.make_async_copy(block, block, direct_recv.at[c, a, part])

    def passed_on(c, a, part):
        block = kv_all.at[a * 2 + core, c, part]
        return pltpu.make_async_remote_copy(
            src_ref=block, dst_ref=block,
            send_sem=forward_send.at[a], recv_sem=sibling_recv.at[c, a, part],
            device_id={"seq": sibling}, device_id_type=MESH,
        )

    def pair(c, part):
        block = kv_all.at[stripe, c, part]
        return pltpu.make_async_remote_copy(
            src_ref=block, dst_ref=block,
            send_sem=pair_send, recv_sem=pair_recv.at[c, part],
            device_id={"seq": sibling}, device_id_type=MESH,
        )

    def settle(ref, sem):
        pltpu.make_async_copy(ref, ref, sem).wait()

    def blend(c, part):
        cols = part_cols(c, part)
        slots = landing[:, :, cols].reshape(n_half * slot_rows, CW)
        x = jnp.dot(pick[...], slots, preferred_element_type=F32)
        x = x + jnp.dot(far_pick[...], far[c, :, part * CW:(part + 1) * CW], preferred_element_type=F32)
        fresh = jnp.dot(fresh_pick[...], fresh_ref[0, :, cols], preferred_element_type=F32)
        if part == 0:
            x = x * cosine[...] + pltpu.roll(x, D_HEAD // 2, 1) * sine[...]
        x = jnp.where(is_fresh[...] > 0.0, fresh, x)
        x = x.astype(jnp.bfloat16)
        kv_all[stripe, c, part] = x
        kv_out[0, :, cols] = x

    scale = math.log2(math.e) / math.sqrt(D_HEAD)
    contract = (((1,), (1,)), ((), ()))

    def forward(c, part):
        for a in range(n_chips - 1):
            @pl.when(a < chip)
            def _():
                direct(c, a, part).wait()
                passed_on(c, a, part).start()

    def await_sibling(c, part):
        for a in range(n_chips - 1):
            @pl.when(a < chip)
            def _():
                settle(kv_all.at[a * 2 + 1 - core, c, part], sibling_recv.at[c, a, part])

        @pl.when(core == 1)
        def _():
            settle(kv_all.at[chip * 2, c, part], pair_recv.at[c, part])

    def peak_of(x):
        top = x[:, :D_HEAD]
        for i in range(1, tok // D_HEAD):
            top = jnp.maximum(top, x[:, i * D_HEAD:(i + 1) * D_HEAD])
        return top

    def attend(c):
        base = c * GROUPS * D_HEAD
        rows = GROUPS * sel

        def queries():
            wide = qv[:, pl.ds(pl.multiple_of(base, GROUPS * D_HEAD), GROUPS * D_HEAD)]
            return jnp.concatenate([wide[:, g * D_HEAD:(g + 1) * D_HEAD] for g in range(GROUPS)], axis=0)

        def scores_of(q, s):
            return lax.dot_general(q, kv_all[s, c, 0], contract, preferred_element_type=F32)

        def weights_of(x, top):
            return jnp.exp2(x * scale - top).astype(jnp.bfloat16)

        def with_ones(v):
            return jnp.concatenate([v, jnp.ones_like(v)], axis=1)

        def group(late):
            q = queries()
            begin = stripe - late
            own = scores_of(q, stripe)
            keep = iota((sel, tok), 1).astype(F32) + first <= limit[:, 0:1]
            keep = jnp.concatenate([jnp.where(keep, 0.0, -1e30)] * GROUPS, axis=0)
            own = jnp.where(keep < 0.0, -1e30, own)
            await_sibling(c, 0)
            found = [scores_of(q, begin + i) for i in range(late)] + [own]
            top = functools.reduce(jnp.maximum, [peak_of(x) for x in found])
            if n_seq > SPAN:
                def score(s, top):
                    x = scores_of(q, s)
                    scores[s] = x
                    return jnp.maximum(top, peak_of(x))

                top = lax.fori_loop(0, begin, score, top)
            top = jnp.max(top, axis=1, keepdims=True) * scale
            weights = jnp.concatenate([weights_of(x, top) for x in found], axis=1)

            @pl.when(c == CHUNKS - 1)
            def _():
                forward(c, 1)

            await_sibling(c, 1)
            values = kv_all[pl.ds(begin, late + 1), c, 1].reshape((late + 1) * tok, D_HEAD)
            acc = jnp.dot(weights, with_ones(values), preferred_element_type=F32)
            if n_seq > SPAN:
                acc = lax.fori_loop(0, begin, lambda s, acc: acc + jnp.dot(
                    weights_of(scores[s], top), with_ones(kv_all[s, c, 1]), preferred_element_type=F32
                ), acc)
            normed = acc[:, :D_HEAD] * (1.0 / acc[:, D_HEAD:])
            live = limit[...] >= 0.0
            for g in range(GROUPS):
                part = jnp.where(live, normed[g * sel:(g + 1) * sel], 0.0)
                attn_out[0, :, pl.ds(pl.multiple_of(base + g * D_HEAD, D_HEAD), D_HEAD)] = part.astype(jnp.bfloat16)

        for late in range(min(n_seq, SPAN)):
            @pl.when(stripe % SPAN == late)
            def _():
                group(late)

    def relay(c):
        for part in range(2):
            settle(relay_in.at[:, pl.ds(0, n_half - 1), :, part_cols(c, part)], relay_recv.at[c, part])

        @pl.when(c == 0)
        def _():
            for j in range(2):
                own_relay(j).wait()

        for j in range(2):
            for part in range(2):
                slots = relay_in[j, :, :, part_cols(c, part)].reshape(n_half * slot_rows, CW)
                rows = jnp.dot(relay_pick[j], slots, preferred_element_type=F32)
                cols = slice(part * CW, (part + 1) * CW)
                merged[j, c, :, cols] = rows[:keep_rows].astype(jnp.bfloat16)
                if spill:
                    tail_out[j, c, :, cols] = rows[keep_rows:].astype(jnp.bfloat16)
            if spill:
                relay_tail(c, j).start()

    def send_on(c):
        if spill:
            settle(tail_in.at[:, c], tail_recv.at[c])
        for j in range(2):
            if spill:
                merged[j, c, keep_rows - spill:] = merged[j, c, keep_rows - spill:] + tail_in[j, c]
            relay_out(c, j).start()

    def step(c, carry):
        def merge(r, carry):
            relay(r)
            send_on(r)
            return carry

        newest = relayed(c) - 1
        merging = is_relay & (newest >= relayed(c - 1))

        @pl.when(merging)
        def _():
            lax.fori_loop(relayed(c - 1), newest, merge, 0)
            relay(newest)

        @pl.when(c > 0)
        def _():
            forward(c - 1, 0)

        @pl.when(merging)
        def _():
            send_on(newest)

        @pl.when(c < CHUNKS)
        def _():
            relay_out(c, 0).wait_recv()
            if spill:
                far_tail(c).start()

        @pl.when((c > 0) & (c < CHUNKS))
        def _():
            forward(c - 1, 1)

        @pl.when(c > 0)
        def _():
            attend(c - 1)

        @pl.when(c < CHUNKS)
        def _():
            @pl.when(c == 0)
            def _():
                own_copy.wait()
                q_copy.wait()

            if spill:
                far_tail(c).wait_recv()

            for part in range(2):
                settle(landing.at[pl.ds(0, n_half - 1), :, part_cols(c, part)], fetch_recv.at[c, part])
                blend(c, part)
                for b in range(1, n_chips):
                    @pl.when(chip < b)
                    def _():
                        gather(c, b, part).start()

                @pl.when(core == 0)
                def _():
                    pair(c, part).start()

        return carry

    lax.fori_loop(0, CHUNKS + 1, step, 0)

    settle(landing.at[pl.ds(0, n_half - 1)], fetch_send)

    @pl.when(is_relay)
    def _():
        settle(relay_in.at[:, pl.ds(0, ny - 1)], relay_send)
        settle(merged, merged_send)
        if spill:
            settle(tail_out, tail_send)

    @pl.when(jnp.logical_not(is_relay))
    def _():
        settle(relay_in.at[:, pl.ds(0, ny)], relay_send)

    if spill:
        settle(tail_in.at[0], spill_send)

    for b in range(1, n_chips):
        @pl.when(chip < b)
        def _():
            settle(kv_all.at[0], gather_send.at[b])

    for a in range(n_chips - 1):
        @pl.when(a < chip)
        def _():
            settle(kv_all.at[0], forward_send.at[a])

    @pl.when(core == 0)
    def _():
        settle(kv_all.at[0], pair_send)


def on_device(n_store, n_seq, store_kv, span_len, span_shard, q_sel, fresh_kv, sel_pos):
    slot_rows = store_kv.shape[1]
    tok = 256
    sel = sel_pos.shape[1]
    half = np.arange(D_HEAD // 2, dtype=np.float64) * 2.0 / D_HEAD
    inverse = np.power(ROPE_BASE, -np.concatenate([half, half]))[None].astype(np.float32)
    hbm = pl.BlockSpec(memory_space=pl.ANY)
    dma = pltpu.SemaphoreType.DMA
    bf16 = jnp.bfloat16
    n_chips = n_seq // 2
    n_half = n_store // 2
    keep_rows = frame_rows(n_store, slot_rows, tok)
    spill = tok - keep_rows
    return pl.pallas_call(
        functools.partial(kernel, n_store, n_seq),
        out_shape=(
            pltpu.VMEM((1, tok, 2 * KV_WIDTH), bf16),
            pltpu.VMEM((1, sel, HEADS * D_HEAD), bf16),
        ),
        in_specs=[hbm] * 7,
        out_specs=(pl.BlockSpec(memory_space=pltpu.VMEM),) * 2,
        scratch_shapes=[
            pltpu.VMEM(span_len.shape, jnp.int32),
            pltpu.VMEM(span_shard.shape, jnp.int32),
            pltpu.VMEM(inverse.shape, F32),
            pltpu.VMEM(fresh_kv.shape, bf16),
            pltpu.VMEM(sel_pos.shape, jnp.int32),
            pltpu.VMEM((n_half, slot_rows, 2 * KV_WIDTH), bf16),
            pltpu.VMEM((2, n_half, slot_rows, 2 * KV_WIDTH), bf16),
            pltpu.VMEM((2, CHUNKS, keep_rows, 2 * CW), bf16),
            pltpu.VMEM((CHUNKS, tok, 2 * CW), bf16),
            pltpu.VMEM((n_seq, CHUNKS, 2, tok, CW), bf16),
            pltpu.VMEM((sel, HEADS * D_HEAD), bf16),
            pltpu.VMEM((max(n_seq - SPAN, 1), GROUPS * sel, tok), F32),
            pltpu.VMEM((tok, n_half * slot_rows), bf16),
            pltpu.VMEM((tok, tok), bf16),
            pltpu.VMEM((2, tok, n_half * slot_rows), bf16),
            pltpu.VMEM((tok, sel), bf16),
            pltpu.VMEM((2, CHUNKS, spill, 2 * CW), bf16),
            pltpu.VMEM((2, CHUNKS, spill, 2 * CW), bf16),
            pltpu.VMEM((tok, D_HEAD), F32),
            pltpu.VMEM((tok, D_HEAD), F32),
            pltpu.VMEM((tok, D_HEAD), F32),
            pltpu.VMEM((sel, D_HEAD), F32),
            dma(()),
            dma((CHUNKS, 2)),
            dma(()),
            dma((CHUNKS, 2)),
            dma(()),
            dma((CHUNKS,)),
            dma(()),
            dma((CHUNKS,)),
            dma(()),
            dma((CHUNKS,)),
            dma((3,)),
            dma(()),
            dma((n_chips,)),
            dma((CHUNKS, n_chips - 1, 2)),
            dma((CHUNKS, n_chips - 1, 2)),
            dma((CHUNKS, 2)),
            dma((n_chips,)),
            dma(()),
            dma((5,)),
        ],
        compiler_params=pltpu.CompilerParams(
            collective_id=0, has_side_effects=True, vmem_limit_bytes=60 * 1024 * 1024
        ),
    )(store_kv, span_len, span_shard, jnp.asarray(inverse), q_sel, fresh_kv, sel_pos)


def solution(mesh):
    n_store, n_seq = mesh.shape["store"], mesh.shape["seq"]
    return jax.shard_map(
        functools.partial(on_device, n_store, n_seq),
        mesh=mesh,
        in_specs=(
            P("store", "seq", None),
            P(),
            P(),
            P("store", "seq", None),
            P("store", "seq", None),
            P("store", "seq"),
        ),
        out_specs=(P("store", "seq", None), P("store", "seq", None)),
        check_vma=False,
    )
```

```python
import functools
import math

import jax
import jax.numpy as jnp
import numpy as np
from jax import lax
from jax.experimental import pallas as pl
from jax.experimental.pallas import tpu as pltpu
from jax.sharding import PartitionSpec as P

HEADS = 64
KV_HEADS = 8
D_HEAD = 128
GROUPS = HEADS // KV_HEADS
KV_WIDTH = KV_HEADS * D_HEAD
ROPE_BASE = 500000.0
CHUNKS = KV_HEADS
LEAD = 3
BURST = 8
SPAN = 4
PIECES = 4
SHORTEST, LONGEST = 37, 80
CW = D_HEAD
F32 = jnp.float32
MESH = pl.DeviceIdType.MESH


def iota(shape, axis):
    return lax.broadcasted_iota(jnp.int32, shape, axis)


def own_row(ref, row):
    table = ref[...].astype(F32)
    return jnp.sum(jnp.where(iota(table.shape, 0) == row, table, 0.0), axis=0, keepdims=True)


def column(row):
    n = row.shape[1]
    square = (n, n)
    return jnp.sum(jnp.where(iota(square, 0) == iota(square, 1), row, 0.0), axis=1, keepdims=True)


def frame_rows(n_store, slot_rows, tok):
    half = n_store // 2
    shortest = slot_rows * SHORTEST // LONGEST
    window = 2 * tok
    most, m = 0, 0
    while window > m * half * shortest:
        most = max(most, min((m + 1) * half * slot_rows, window - m * half * shortest))
        m += 1
    return min(tok, -(-most // 32) * 16)


def kernel(
    n_store, n_seq,
    store_ref, len_hbm, shard_hbm, inv_hbm, q_ref, fresh_hbm, sel_hbm,
    kv_out, attn_out,
    len_ref, shard_ref, inv_ref, fresh_ref, sel_ref,
    landing, relay_in, merged, far, kv_all, qv, scores, pick, far_pick, relay_pick, fresh_pick, tail_out, tail_in, is_fresh, cosine, sine, limit,
    fetch_send, fetch_recv, relay_send, relay_recv, merged_send, far_recv,
    tail_send, tail_recv, spill_send, spill_recv,
    own_sem, q_sem, gather_send, direct_recv, sibling_recv, pair_recv,
    forward_send, pair_send, load_sem,
):
    me = lax.axis_index("store")
    stripe = lax.axis_index("seq")
    slot_rows = store_ref.shape[1]
    tok = kv_out.shape[1]
    sel = sel_ref.shape[1]
    keep_rows = merged.shape[2]
    spill = tok - keep_rows
    n_chips = n_seq // 2
    chip = stripe // 2
    core = stripe % 2
    sibling = chip * 2 + (1 - core)
    n_half = n_store // 2
    ny = n_store // 4
    half = me // n_half
    local = me % n_half
    lane = me % ny
    relay_row = 1 + half
    is_relay = me // ny == relay_row

    barrier = pltpu.get_barrier_semaphore()
    for d in range(1, n_half):
        peer = half * n_half + (local + d) % n_half
        pl.semaphore_signal(barrier, inc=1, device_id={"store": peer}, device_id_type=MESH)
    pl.semaphore_signal(barrier, inc=1, device_id={"store": (2 - half) * ny + lane}, device_id_type=MESH)
    for d in range(1, n_seq):
        pl.semaphore_signal(barrier, inc=1, device_id={"seq": (stripe + d) % n_seq}, device_id_type=MESH)

    loads = [
        pltpu.make_async_copy(src, dst, load_sem.at[i])
        for i, (src, dst) in enumerate([
            (len_hbm, len_ref), (shard_hbm, shard_ref), (inv_hbm, inv_ref), (sel_hbm, sel_ref), (fresh_hbm, fresh_ref),
        ])
    ]
    for load in loads:
        load.start()

    peers = n_half + n_seq - 2

    @pl.when(is_relay)
    def _():
        pl.semaphore_wait(barrier, peers + 2)

    @pl.when(jnp.logical_not(is_relay))
    def _():
        pl.semaphore_wait(barrier, peers)

    def part_cols(c, part):
        return pl.ds(pl.multiple_of(part * KV_WIDTH + c * CW, CW), CW)

    def fetch(c, src, dst, part):
        cols = part_cols(c, part)
        return pltpu.make_async_remote_copy(
            src_ref=store_ref.at[half * n_half + dst, :, cols],
            dst_ref=landing.at[src, :, cols],
            send_sem=fetch_send,
            recv_sem=fetch_recv.at[c, part],
            device_id={"store": half * n_half + dst},
            device_id_type=MESH,
        )

    def far_request(y, j):
        return ((1 - half) * 2 + j) * ny + y

    def to_relay(c, src, y, j, part):
        cols = part_cols(c, part)
        return pltpu.make_async_remote_copy(
            src_ref=store_ref.at[far_request(y, j), :, cols],
            dst_ref=relay_in.at[j, src, :, cols],
            send_sem=relay_send,
            recv_sem=relay_recv.at[c, part],
            device_id={"store": relay_row * ny + y},
            device_id_type=MESH,
        )

    def relay_out(c, j):
        return pltpu.make_async_remote_copy(
            src_ref=merged.at[j, c],
            dst_ref=far.at[c, pl.ds(0, keep_rows)],
            send_sem=merged_send,
            recv_sem=far_recv.at[c],
            device_id={"store": far_request(lane, j)},
            device_id_type=MESH,
        )

    def relay_tail(c, j):
        return pltpu.make_async_remote_copy(
            src_ref=tail_out.at[j, c],
            dst_ref=tail_in.at[j, c],
            send_sem=tail_send,
            recv_sem=tail_recv.at[c],
            device_id={"seq": sibling},
            device_id_type=MESH,
        )

    def far_tail(c):
        return pltpu.make_async_remote_copy(
            src_ref=far.at[c, pl.ds(keep_rows - spill, spill)],
            dst_ref=far.at[c, pl.ds(keep_rows, spill)],
            send_sem=spill_send,
            recv_sem=spill_recv.at[c],
            device_id={"seq": sibling},
            device_id_type=MESH,
        )

    own_copy = pltpu.make_async_copy(store_ref.at[me], landing.at[local], own_sem.at[0])
    q_copy = pltpu.make_async_copy(q_ref.at[0], qv, q_sem)

    def own_relay(j):
        return pltpu.make_async_copy(
            store_ref.at[far_request(lane, j)], relay_in.at[j, local], own_sem.at[1 + j]
        )

    def each_to_relay(c, act):
        for j in range(2):
            for part in range(2):
                @pl.when(jnp.logical_not(is_relay))
                def _():
                    act(to_relay(c, local, lane, j, part))

                for d in range(1, ny):
                    act(to_relay(c, local, (lane + d) % ny, j, part))

    def relayed(c):
        return jnp.where(c < 0, 0, jnp.where(c < BURST, jnp.minimum(c + LEAD, CHUNKS), CHUNKS))

    def issue(c, carry):
        def feed(r, carry):
            each_to_relay(r, lambda copy: copy.start())
            return carry

        lax.fori_loop(relayed(c - 1), relayed(c), feed, 0)
        for d in range(1, n_half):
            for part in range(2):
                fetch(c, local, (local + d) % n_half, part).start()
        return carry

    lax.fori_loop(0, CHUNKS, issue, 0)
    own_copy.start()

    @pl.when(is_relay)
    def _():
        for j in range(2):
            own_relay(j).start()

    q_copy.start()

    for load in loads:
        load.wait()

    first = (stripe * tok).astype(F32)
    n_span = len_ref.shape[1]

    def locate(request):
        lengths = own_row(len_ref, request)
        square = (n_span, n_span)
        starts = jnp.sum(
            jnp.where(iota(square, 0) < iota(square, 1), column(lengths), 0.0), axis=0, keepdims=True
        )
        shards = column(own_row(shard_ref, request))
        spread = (n_store, n_span)
        holders = jnp.sum(
            jnp.where(iota(spread, 1) % n_store == iota(spread, 0), shards, 0.0), axis=0, keepdims=True
        )
        grid = (tok, n_span)
        position = iota(grid, 0).astype(F32) + first
        which = jnp.sum(jnp.where(position >= starts, 1.0, 0.0), axis=1, keepdims=True) - 1.0
        picked = iota(grid, 1).astype(F32) == which
        holder = jnp.sum(jnp.where(picked, holders, 0.0), axis=1, keepdims=True)
        start = jnp.sum(jnp.where(picked, starts, 0.0), axis=1, keepdims=True)
        row = iota((tok, 1), 0).astype(F32) + first - jnp.maximum(start, first)
        target = (holder - (half * n_half).astype(F32)) * slot_rows + row
        chosen = jnp.where(iota(pick.shape, 1).astype(F32) == target, 1.0, 0.0)
        side = jnp.where(holder >= n_half, 1.0, 0.0)
        return chosen.astype(jnp.bfloat16), start, jnp.where(side == half.astype(F32), 1.0, 0.0)

    def framed(member):
        square = (tok, tok)
        before = jnp.where(iota(square, 1) < iota(square, 0), 1.0, 0.0).astype(jnp.bfloat16)
        wide = jnp.broadcast_to(member, (tok, D_HEAD)).astype(jnp.bfloat16)
        rank = jnp.dot(before, wide, preferred_element_type=F32)[:, 0:1]
        at = jnp.where(rank < keep_rows, rank, float(2 * keep_rows + spill - 1) - rank)
        at = jnp.where(member > 0.0, at, -1.0)
        return jnp.where(iota(square, 1).astype(F32) == at, 1.0, 0.0).astype(jnp.bfloat16)

    @pl.when(is_relay)
    def _():
        for j in range(2):
            chosen, _, member = locate(far_request(lane, j))
            relay_pick[j] = lax.dot_general(
                framed(member), chosen, (((0,), (0,)), ((), ())), preferred_element_type=F32
            ).astype(jnp.bfloat16)

    near, start, member = locate(me)
    pick[...] = near
    far_pick[...] = framed(1.0 - member)
    angle = start * inv_ref[...]
    cosine[...] = jnp.cos(angle)
    sine[...] = jnp.sin(angle) * jnp.where(iota((1, D_HEAD), 1) < D_HEAD // 2, -1.0, 1.0)
    chosen = sel_ref[...].astype(F32)
    matches = jnp.where(iota((tok, sel), 0).astype(F32) + first == chosen, 1.0, 0.0)
    fresh_pick[...] = matches.astype(jnp.bfloat16)
    is_fresh[...] = jnp.broadcast_to(jnp.sum(matches, axis=1, keepdims=True), is_fresh.shape)
    limit[...] = jnp.broadcast_to(column(chosen), limit.shape)

    def gather(c, peer_chip, part):
        block = kv_all.at[stripe, c, part]
        return pltpu.make_async_remote_copy(
            src_ref=block, dst_ref=block,
            send_sem=gather_send.at[peer_chip], recv_sem=direct_recv.at[c, chip, part],
            device_id={"seq": peer_chip * 2 + core}, device_id_type=MESH,
        )

    def direct(c, a, part):
        block = kv_all.at[a * 2 + core, c, part]
        return pltpu.make_async_copy(block, block, direct_recv.at[c, a, part])

    def passed_on(c, a, part):
        block = kv_all.at[a * 2 + core, c, part]
        return pltpu.make_async_remote_copy(
            src_ref=block, dst_ref=block,
            send_sem=forward_send.at[a], recv_sem=sibling_recv.at[c, a, part],
            device_id={"seq": sibling}, device_id_type=MESH,
        )

    def pair(c, part):
        block = kv_all.at[stripe, c, part]
        return pltpu.make_async_remote_copy(
            src_ref=block, dst_ref=block,
            send_sem=pair_send, recv_sem=pair_recv.at[c, part],
            device_id={"seq": sibling}, device_id_type=MESH,
        )

    def settle(ref, sem):
        pltpu.make_async_copy(ref, ref, sem).wait()

    def blend(c, part):
        cols = part_cols(c, part)
        slots = landing[:, :, cols].reshape(n_half * slot_rows, CW)
        x = jnp.dot(pick[...], slots, preferred_element_type=F32)
        x = x + jnp.dot(far_pick[...], far[c, :, part * CW:(part + 1) * CW], preferred_element_type=F32)
        fresh = jnp.dot(fresh_pick[...], fresh_ref[0, :, cols], preferred_element_type=F32)
        if part == 0:
            x = x * cosine[...] + pltpu.roll(x, D_HEAD // 2, 1) * sine[...]
        x = jnp.where(is_fresh[...] > 0.0, fresh, x)
        x = x.astype(jnp.bfloat16)
        kv_all[stripe, c, part] = x
        kv_out[0, :, cols] = x

    scale = math.log2(math.e) / math.sqrt(D_HEAD)
    contract = (((1,), (1,)), ((), ()))

    def forward(c, part):
        for a in range(n_chips - 1):
            @pl.when(a < chip)
            def _():
                direct(c, a, part).wait()
                passed_on(c, a, part).start()

    def await_sibling(c, part):
        for a in range(n_chips - 1):
            @pl.when(a < chip)
            def _():
                settle(kv_all.at[a * 2 + 1 - core, c, part], sibling_recv.at[c, a, part])

        @pl.when(core == 1)
        def _():
            settle(kv_all.at[chip * 2, c, part], pair_recv.at[c, part])

    def peak_of(x):
        top = x[:, :D_HEAD]
        for i in range(1, tok // D_HEAD):
            top = jnp.maximum(top, x[:, i * D_HEAD:(i + 1) * D_HEAD])
        return top

    def attend(c):
        base = c * GROUPS * D_HEAD
        rows = GROUPS * sel

        def queries():
            wide = qv[:, pl.ds(pl.multiple_of(base, GROUPS * D_HEAD), GROUPS * D_HEAD)]
            return jnp.concatenate([wide[:, g * D_HEAD:(g + 1) * D_HEAD] for g in range(GROUPS)], axis=0)

        def scores_of(q, s):
            return lax.dot_general(q, kv_all[s, c, 0], contract, preferred_element_type=F32)

        def weights_of(x, top):
            return jnp.exp2(x * scale - top).astype(jnp.bfloat16)

        def with_ones(v):
            return jnp.concatenate([v, jnp.ones_like(v)], axis=1)

        def group(late):
            q = queries()
            begin = stripe - late
            own = scores_of(q, stripe)
            keep = iota((sel, tok), 1).astype(F32) + first <= limit[:, 0:1]
            keep = jnp.concatenate([jnp.where(keep, 0.0, -1e30)] * GROUPS, axis=0)
            own = jnp.where(keep < 0.0, -1e30, own)
            await_sibling(c, 0)
            found = [scores_of(q, begin + i) for i in range(late)] + [own]
            top = functools.reduce(jnp.maximum, [peak_of(x) for x in found])
            if n_seq > SPAN:
                def score(s, top):
                    x = scores_of(q, s)
                    scores[s] = x
                    return jnp.maximum(top, peak_of(x))

                top = lax.fori_loop(0, begin, score, top)
            top = jnp.max(top, axis=1, keepdims=True) * scale
            weights = jnp.concatenate([weights_of(x, top) for x in found], axis=1)

            @pl.when(c == CHUNKS - 1)
            def _():
                forward(c, 1)

            await_sibling(c, 1)
            values = kv_all[pl.ds(begin, late + 1), c, 1].reshape((late + 1) * tok, D_HEAD)
            acc = jnp.dot(weights, with_ones(values), preferred_element_type=F32)
            if n_seq > SPAN:
                acc = lax.fori_loop(0, begin, lambda s, acc: acc + jnp.dot(
                    weights_of(scores[s], top), with_ones(kv_all[s, c, 1]), preferred_element_type=F32
                ), acc)
            normed = acc[:, :D_HEAD] * (1.0 / acc[:, D_HEAD:])
            live = limit[...] >= 0.0
            for g in range(GROUPS):
                part = jnp.where(live, normed[g * sel:(g + 1) * sel], 0.0)
                attn_out[0, :, pl.ds(pl.multiple_of(base + g * D_HEAD, D_HEAD), D_HEAD)] = part.astype(jnp.bfloat16)

        for late in range(min(n_seq, SPAN)):
            @pl.when(stripe % SPAN == late)
            def _():
                group(late)

    def relay(c):
        for part in range(2):
            settle(relay_in.at[:, pl.ds(0, n_half - 1), :, part_cols(c, part)], relay_recv.at[c, part])

        @pl.when(c == 0)
        def _():
            for j in range(2):
                own_relay(j).wait()

        for j in range(2):
            slots = jnp.concatenate([
                relay_in[j, :, :, part_cols(c, part)].reshape(n_half * slot_rows, CW) for part in range(2)
            ], axis=1)
            rows = jnp.dot(relay_pick[j], slots, preferred_element_type=F32)
            merged[j, c] = rows[:keep_rows].astype(jnp.bfloat16)
            if spill:
                tail_out[j, c] = rows[keep_rows:].astype(jnp.bfloat16)
            if spill:
                relay_tail(c, j).start()

    def send_on(c):
        if spill:
            settle(tail_in.at[:, c], tail_recv.at[c])
        for j in range(2):
            if spill:
                merged[j, c, keep_rows - spill:] = merged[j, c, keep_rows - spill:] + tail_in[j, c]
            relay_out(c, j).start()

    def step(c, carry):
        def merge(r, carry):
            relay(r)
            send_on(r)
            return carry

        newest = relayed(c) - 1
        merging = is_relay & (newest >= relayed(c - 1))

        @pl.when(merging)
        def _():
            lax.fori_loop(relayed(c - 1), newest, merge, 0)
            relay(newest)

        @pl.when(c > 0)
        def _():
            forward(c - 1, 0)

        @pl.when(merging)
        def _():
            send_on(newest)

        @pl.when(c < CHUNKS)
        def _():
            relay_out(c, 0).wait_recv()
            if spill:
                far_tail(c).start()

        @pl.when((c > 0) & (c < CHUNKS))
        def _():
            forward(c - 1, 1)

        @pl.when(c < CHUNKS)
        def _():
            @pl.when(c == 0)
            def _():
                own_copy.wait()
                q_copy.wait()

            if spill:
                far_tail(c).wait_recv()

            for part in range(2):
                settle(landing.at[pl.ds(0, n_half - 1), :, part_cols(c, part)], fetch_recv.at[c, part])
                blend(c, part)
                for b in range(1, n_chips):
                    @pl.when(chip < b)
                    def _():
                        gather(c, b, part).start()

                @pl.when(core == 0)
                def _():
                    pair(c, part).start()

        @pl.when(c > 0)
        def _():
            attend(c - 1)

        return carry

    lax.fori_loop(0, CHUNKS + 1, step, 0)

    settle(landing.at[pl.ds(0, n_half - 1)], fetch_send)

    @pl.when(is_relay)
    def _():
        settle(relay_in.at[:, pl.ds(0, ny - 1)], relay_send)
        settle(merged, merged_send)
        if spill:
            settle(tail_out, tail_send)

    @pl.when(jnp.logical_not(is_relay))
    def _():
        settle(relay_in.at[:, pl.ds(0, ny)], relay_send)

    if spill:
        settle(tail_in.at[0], spill_send)

    for b in range(1, n_chips):
        @pl.when(chip < b)
        def _():
            settle(kv_all.at[0], gather_send.at[b])

    for a in range(n_chips - 1):
        @pl.when(a < chip)
        def _():
            settle(kv_all.at[0], forward_send.at[a])

    @pl.when(core == 0)
    def _():
        settle(kv_all.at[0], pair_send)


def write_out(kv_ref, attn_ref, kv_out, attn_out, sems):
    copies = []
    for i, (src, dst) in enumerate(((kv_ref, kv_out), (attn_ref, attn_out))):
        rows = src.shape[1] // PIECES
        for p in range(PIECES):
            at = pl.ds(p * rows, rows)
            copies.append(pltpu.make_async_copy(src.at[0, at], dst.at[0, at], sems.at[i, p]))
    for copy in copies:
        copy.start()
    for copy in copies:
        copy.wait()


def on_device(n_store, n_seq, store_kv, span_len, span_shard, q_sel, fresh_kv, sel_pos):
    slot_rows = store_kv.shape[1]
    tok = 256
    sel = sel_pos.shape[1]
    half = np.arange(D_HEAD // 2, dtype=np.float64) * 2.0 / D_HEAD
    inverse = np.power(ROPE_BASE, -np.concatenate([half, half]))[None].astype(np.float32)
    hbm = pl.BlockSpec(memory_space=pl.ANY)
    dma = pltpu.SemaphoreType.DMA
    bf16 = jnp.bfloat16
    n_chips = n_seq // 2
    n_half = n_store // 2
    keep_rows = frame_rows(n_store, slot_rows, tok)
    spill = tok - keep_rows
    kv, attn = pl.pallas_call(
        functools.partial(kernel, n_store, n_seq),
        out_shape=(
            pltpu.VMEM((1, tok, 2 * KV_WIDTH), bf16),
            pltpu.VMEM((1, sel, HEADS * D_HEAD), bf16),
        ),
        in_specs=[hbm] * 7,
        out_specs=(pl.BlockSpec(memory_space=pltpu.VMEM),) * 2,
        scratch_shapes=[
            pltpu.VMEM(span_len.shape, jnp.int32),
            pltpu.VMEM(span_shard.shape, jnp.int32),
            pltpu.VMEM(inverse.shape, F32),
            pltpu.VMEM(fresh_kv.shape, bf16),
            pltpu.VMEM(sel_pos.shape, jnp.int32),
            pltpu.VMEM((n_half, slot_rows, 2 * KV_WIDTH), bf16),
            pltpu.VMEM((2, n_half, slot_rows, 2 * KV_WIDTH), bf16),
            pltpu.VMEM((2, CHUNKS, keep_rows, 2 * CW), bf16),
            pltpu.VMEM((CHUNKS, tok, 2 * CW), bf16),
            pltpu.VMEM((n_seq, CHUNKS, 2, tok, CW), bf16),
            pltpu.VMEM((sel, HEADS * D_HEAD), bf16),
            pltpu.VMEM((max(n_seq - SPAN, 1), GROUPS * sel, tok), F32),
            pltpu.VMEM((tok, n_half * slot_rows), bf16),
            pltpu.VMEM((tok, tok), bf16),
            pltpu.VMEM((2, tok, n_half * slot_rows), bf16),
            pltpu.VMEM((tok, sel), bf16),
            pltpu.VMEM((2, CHUNKS, spill, 2 * CW), bf16),
            pltpu.VMEM((2, CHUNKS, spill, 2 * CW), bf16),
            pltpu.VMEM((tok, D_HEAD), F32),
            pltpu.VMEM((tok, D_HEAD), F32),
            pltpu.VMEM((tok, D_HEAD), F32),
            pltpu.VMEM((sel, D_HEAD), F32),
            dma(()),
            dma((CHUNKS, 2)),
            dma(()),
            dma((CHUNKS, 2)),
            dma(()),
            dma((CHUNKS,)),
            dma(()),
            dma((CHUNKS,)),
            dma(()),
            dma((CHUNKS,)),
            dma((3,)),
            dma(()),
            dma((n_chips,)),
            dma((CHUNKS, n_chips - 1, 2)),
            dma((CHUNKS, n_chips - 1, 2)),
            dma((CHUNKS, 2)),
            dma((n_chips,)),
            dma(()),
            dma((5,)),
        ],
        compiler_params=pltpu.CompilerParams(
            collective_id=0, has_side_effects=True, vmem_limit_bytes=60 * 1024 * 1024
        ),
    )(store_kv, span_len, span_shard, jnp.asarray(inverse), q_sel, fresh_kv, sel_pos)
    return pl.pallas_call(
        write_out,
        out_shape=(jax.ShapeDtypeStruct(kv.shape, bf16), jax.ShapeDtypeStruct(attn.shape, bf16)),
        in_specs=[pl.BlockSpec(memory_space=pltpu.VMEM)] * 2,
        out_specs=(hbm, hbm),
        scratch_shapes=[dma((2, PIECES))],
        compiler_params=pltpu.CompilerParams(has_side_effects=True),
    )(*(pltpu.with_memory_space_constraint(x, pltpu.VMEM) for x in (kv, attn)))


def solution(mesh):
    n_store, n_seq = mesh.shape["store"], mesh.shape["seq"]
    return jax.shard_map(
        functools.partial(on_device, n_store, n_seq),
        mesh=mesh,
        in_specs=(
            P("store", "seq", None),
            P(),
            P(),
            P("store", "seq", None),
            P("store", "seq", None),
            P("store", "seq"),
        ),
        out_specs=(P("store", "seq", None), P("store", "seq", None)),
        check_vma=False,
    )
```
